32 devices in a mesh: blk: 16 (over z, x, core), tp: 2 (over y).
Axes of the slice: x: 2, y: 2, z: 4, core: 2. Of those that a mesh axis runs over, the one named last changes fastest.
Arguments:
- weights: float32 [16, 1024, 1024], P('blk', None, 'tp'), may hold values from -6 to 6
- copies: bfloat16 [16, 1024, 1024], P('blk', None, 'tp'), may hold values from -60 to 60
- copies_mixed: bfloat16 [16, 1024, 1024], P('blk', None, 'tp'), may hold values from -64 to 64
- tracker: bfloat16 [16, 1024, 1024], P('blk', None, 'tp'), may hold values from -6 to 6
- tracker_copy: bfloat16 [16, 1024, 1024], P('blk', None, 'tp'), may hold values from -6 to 6
- tracker_mixed: bfloat16 [16, 1024, 1024], P('blk', None, 'tp'), may hold values from -6 to 6
- grad_prev: bfloat16 [16, 1024, 1024], P('blk', None, 'tp'), may hold values from -3 to 3
- tokens: bfloat16 [16, 1024, 1024], P('blk', 'tp'), may hold values from -12 to 12
- image_ids: int32 [16, 1024], P('blk'), may hold values from 0 to 5, never falling along the last dimension, each value on 1 to 197 neighbouring positions
- key_weight: bfloat16 [1024, 1024], P(None, 'tp'), may hold values from -0.1875 to 0.1875
- value_weight: bfloat16 [1024, 1024], P(None, 'tp'), may hold values from -0.1875 to 0.1875
- out_grad: bfloat16 [16, 1024, 1024], P('blk', None, 'tp'), may hold values from -48 to 48
- row_picks: int32 [16, 2, 64], replicated, may hold values from 0 to 1023, as said below
Outputs:
- weights_new: float32 [16, 1024, 1024], P('blk', None, 'tp')
- copies_new: bfloat16 [16, 1024, 1024], P('blk', None, 'tp')
- mixed_new: bfloat16 [16, 1024, 1024], P('blk', None, 'tp')
- tracker_new: bfloat16 [16, 1024, 1024], P('blk', None, 'tp')
- tracker_copy_new: bfloat16 [16, 1024, 1024], P('blk', None, 'tp')
- tracker_mixed_new: bfloat16 [16, 1024, 1024], P('blk', None, 'tp')
- grad_new: bfloat16 [16, 1024, 1024], P('blk', None, 'tp')
- consensus: float32 [], replicated
The draws below stay inside these ranges and needn't reach their ends.
Inputs may be any that keep to these rules, and one draw needn't show every extreme that they name: `image_ids`: never falling along a replica's tokens; an image holds 1 to 197 tokens. `row_picks`: each row lists 64 different rows; the same picks serve every head shard of a replica.
All inputs are finite; a program needn't handle non-finite values.
Results may differ from the reference program's by a relative error of at most 0.0095.
The reference program's roundings to bfloat16 on the way (of `query_weight`, `score_grad` and `query_grad`) count: a program that leaves them out, or rounds other values in their place, can miss the bound.
Values may be sent and summed in bfloat16 or wider, within the bound.
A program may use at most 128 MiB of HBM per device.

```python
import math
import jax
import jax.numpy as jnp
import numpy as np
from jax import lax

D = 1024
HEADS = 16
HD = 64
SEG_MOST = 197
ROWS = 1024
KBLK = 64
IMGS = 6
N_BLK = 16


def key_matrix(key):
    noise_key = jax.random.fold_in(key, 7002)
    base = jnp.clip(jax.random.normal(noise_key, (D, D), jnp.float32), -6.0, 6.0)
    return (base * D ** (-0.5)).astype(jnp.bfloat16)


def draw_key_weight(key, part):
    return key_matrix(key)


def draw_weights(key, part):
    own_key = jax.random.fold_in(key, 7003)
    full_shape = (N_BLK, D, D)
    return jnp.clip(jax.random.normal(own_key, full_shape, jnp.float32), -6.0, 6.0)


def draw_tokens(key, part):
    own_key = jax.random.fold_in(key, 7004)
    normal_key = jax.random.fold_in(own_key, 0)
    full_shape = (N_BLK, ROWS, D)
    values = jax.random.normal(normal_key, full_shape, jnp.float32)
    return jnp.clip(values, -6.0, 6.0).astype(jnp.bfloat16)


def copy_fields(key):
    base_key = jax.random.fold_in(key, 7010)
    keys_all = jax.random.split(base_key, 8)
    full_shape = (N_BLK, D, D)
    replica = jnp.arange(N_BLK, dtype=jnp.float32)
    level = (1.0 + 2.0 * replica / max(N_BLK - 1, 1)) * jnp.exp(jax.random.uniform(keys_all[0], (N_BLK,), jnp.float32) * jnp.log(1.5))
    column = jnp.arange(D, dtype=jnp.float32) / max(D - 1, 1)
    group_count = D // 16
    rise_groups = jnp.repeat(jnp.exp(jax.random.uniform(keys_all[2], (group_count,), jnp.float32) * jnp.log(2.0)), 16)
    fall_groups = jnp.repeat(jnp.exp(jax.random.uniform(keys_all[3], (group_count,), jnp.float32) * jnp.log(2.0)), 16)
    rising = jnp.exp(jnp.log(6.0) * column) * rise_groups
    falling = jnp.exp(jnp.log(6.0) * (1.0 - column)) * fall_groups
    copy_rows = jnp.exp(jax.random.uniform(keys_all[4], (N_BLK, D, 1), jnp.float32) * jnp.log(3.0))
    gap_rows = jnp.exp(jax.random.uniform(keys_all[5], (N_BLK, D, 1), jnp.float32) * jnp.log(3.0))
    copy_noise = jnp.clip(jax.random.normal(keys_all[6], full_shape, jnp.float32), -4.0, 4.0)
    gap_noise = jnp.clip(jax.random.normal(keys_all[7], full_shape, jnp.float32), -4.0, 4.0)
    copies_value = jnp.clip(0.15 * level[:, None, None] * copy_rows * rising[None, None, :] * copy_noise, -60.0, 60.0)
    gap_value = 0.02 * level[:, None, None] * gap_rows * falling[None, None, :] * gap_noise
    mixed_value = jnp.clip(copies_value + gap_value, -64.0, 64.0)
    return (copies_value, mixed_value)


def draw_copies(key, part):
    copies_value, mixed_value = copy_fields(key)
    return copies_value.astype(jnp.bfloat16)


def draw_copies_mixed(key, part):
    copies_value, mixed_value = copy_fields(key)
    return mixed_value.astype(jnp.bfloat16)


def draw_row_picks(key, part):
    own_key = jax.random.fold_in(key, 7006)
    keys_all = jax.random.split(own_key, N_BLK * 2)
    picked = jax.vmap(lambda single: jax.random.permutation(single, D)[:KBLK])(keys_all)
    return picked.reshape(N_BLK, 2, KBLK).astype(jnp.int32)


def shard_levels(rng, extent, pieces, least, largest):
    def one(dim, parts):
        draws = jax.random.uniform(jax.random.fold_in(jax.random.fold_in(rng, 6), dim), (parts,), jnp.float32, least / len(pieces), largest / len(pieces))
        return jnp.repeat(jnp.exp(draws), extent[dim] // parts).reshape((-1,) + (1,) * (len(extent) - dim - 1))

    factor_of = one(*pieces[0])
    for cut in pieces[1:]:
        factor_of = factor_of * one(*cut)
    return factor_of


def length_profile(amount, total, reach, slope):
    portions = [(1 << 20) // math.isqrt(grade ** slope) + 1 for grade in range(2, amount + 1)]
    surplus, counts = total - reach - (amount - 1), [1] * (amount - 1)
    while surplus > 0:
        free = [i for i in range(amount - 1) if counts[i] < reach]
        mass, remaining = sum([portions[i] for i in free]), surplus
        for i in free:
            extra = min(reach - counts[i], max(1, remaining * portions[i] // mass), surplus)
            counts[i] = counts[i] + extra
            surplus = surplus - extra
    return np.array([reach] + counts)


def ragged(key, number_of, total, bound, slope):
    if number_of == 2:
        one = jax.random.randint(key, (), max(1, total - bound), min(bound, total - 1) + 1)
        return jnp.stack([one, total - one])
    lengths = jnp.asarray(length_profile(number_of, total, bound, slope), jnp.int32)
    twos = (number_of - 1) // 2
    giver, taker = lengths[1:1 + 2 * twos:2], lengths[2:2 + 2 * twos:2]
    margin = jnp.minimum(giver - 1, bound - taker)
    passed = jax.random.randint(jax.random.fold_in(key, 1), (twos,), 0, 1 << 20) % (margin + 1)
    lengths = lengths.at[1:1 + 2 * twos:2].set(giver - passed).at[2:2 + 2 * twos:2].set(taker + passed)
    return lengths[jax.random.permutation(jax.random.fold_in(key, 2), number_of)]


def normal_values(key, extent, scale, reach, pieces=(), held_as=jnp.bfloat16):
    gain = shard_levels(key, extent, pieces, -0.22, 0.18) if pieces else 1.0
    result = jax.random.normal(key, extent, jnp.float32) * scale * gain
    return jnp.minimum(jnp.maximum(result, -reach), reach).astype(held_as)


def setup_inputs(seed: int = 0) -> dict:
    key_list = jax.random.split(jax.random.key(seed), 14)
    weights = draw_weights(jax.random.fold_in(key_list[13], 71), 0)
    copies = draw_copies(jax.random.fold_in(key_list[13], 71), 0)
    copies_mixed = draw_copies_mixed(jax.random.fold_in(key_list[13], 71), 0)
    tracker = normal_values(key_list[3], (N_BLK, D, D), 1.0, 6.0, ((0, 16), (2, 2)))
    tracker_copy = normal_values(key_list[4], (N_BLK, D, D), 1.0, 6.0, ((0, 16), (2, 2)))
    tracker_mixed = normal_values(key_list[5], (N_BLK, D, D), 1.0, 6.0, ((0, 16), (2, 2)))
    grad_prev = normal_values(key_list[6], (N_BLK, D, D), 0.5, 3.0, ((0, 16), (2, 2)))
    tokens = draw_tokens(jax.random.fold_in(key_list[13], 71), 0)
    image_ids = jax.vmap(lambda own: jnp.searchsorted(jnp.cumsum(ragged(own, IMGS, ROWS, SEG_MOST, 0)), jnp.arange(ROWS), side="right"))(jax.random.split(key_list[8], N_BLK)).reshape((N_BLK, ROWS)).astype(jnp.int32)
    key_weight = draw_key_weight(jax.random.fold_in(key_list[13], 71), 0)
    value_weight = normal_values(key_list[10], (D, D), D ** -0.5, 0.1875, ((1, 2),))
    out_grad = normal_values(key_list[11], (N_BLK, ROWS, D), 8.0, 48.0, ((0, 16), (2, 2)))
    row_picks = draw_row_picks(jax.random.fold_in(key_list[13], 71), 0)
    return dict(weights=weights, copies=copies, copies_mixed=copies_mixed, tracker=tracker, tracker_copy=tracker_copy, tracker_mixed=tracker_mixed, grad_prev=grad_prev, tokens=tokens, image_ids=image_ids, key_weight=key_weight, value_weight=value_weight, out_grad=out_grad, row_picks=row_picks)


mixing_rate = 0.2
step_rate = 0.5

def contract(left, right, left_dim, right_dim):
    return lax.dot_general(left.astype(jnp.float32), right.astype(jnp.float32), (((left_dim,), (right_dim,)), ((), ())), preferred_element_type=jnp.float32)

def pick_matrix(picks):
    columns = jnp.arange(D, dtype=jnp.int32)
    return (picks[:, None] == columns[None, :]).astype(jnp.float32)

def compress(picks, field):
    matrix = pick_matrix(picks)
    kept = jnp.dot(matrix, field, precision=lax.Precision.HIGHEST)
    return jnp.dot(matrix.T, kept, precision=lax.Precision.HIGHEST)

def gossip_mix(update):
    return (jnp.roll(update, 1, axis=0) + update + jnp.roll(update, -1, axis=0)) / 3.0

def head_grad(query_head, key_head, value_head, out_head, same_image):
    scores = contract(query_head, key_head, 1, 1) * HD ** (-0.5)
    scores = jnp.where(same_image, scores, -1e+30)
    row_max = lax.optimization_barrier(jnp.max(scores, axis=-1, keepdims=True))
    exponent = jnp.exp(scores - row_max)
    attention = exponent / lax.optimization_barrier(jnp.sum(exponent, axis=-1, keepdims=True))
    out_proj = contract(out_head, value_head, 1, 1)
    centred = out_proj - lax.optimization_barrier(jnp.sum(attention * out_proj, axis=-1, keepdims=True))
    score_grad = (attention * centred * HD ** (-0.5)).astype(jnp.bfloat16)
    return jnp.dot(score_grad.astype(jnp.float32), key_head.astype(jnp.float32), preferred_element_type=jnp.float32).astype(jnp.bfloat16)

def replica_grad(weights_row, token_rows, image_row, out_rows, key_weight, value_weight):
    query_weight = (weights_row * D ** (-0.5)).astype(jnp.bfloat16)
    queries = jnp.dot(token_rows.astype(jnp.float32), query_weight.astype(jnp.float32), preferred_element_type=jnp.float32).astype(jnp.bfloat16)
    keyed = jnp.dot(token_rows.astype(jnp.float32), key_weight.astype(jnp.float32), preferred_element_type=jnp.float32).astype(jnp.bfloat16)
    valued = jnp.dot(token_rows.astype(jnp.float32), value_weight.astype(jnp.float32), preferred_element_type=jnp.float32).astype(jnp.bfloat16)
    same_image = image_row[:, None] == image_row[None, :]
    pieces_list = []
    for head_index in range(HEADS):
        low_col = head_index * HD
        pieces_list.append(head_grad(queries[:, low_col:low_col + HD], keyed[:, low_col:low_col + HD], valued[:, low_col:low_col + HD], out_rows[:, low_col:low_col + HD], same_image))
    query_grad = jnp.concatenate(pieces_list, axis=1)
    return (contract(token_rows, query_grad, 0, 0) * D ** (-0.5)).astype(jnp.bfloat16)

def reference(weights, copies, copies_mixed, tracker, tracker_copy, tracker_mixed, grad_prev, tokens, image_ids, key_weight, value_weight, out_grad, row_picks):
    copy_value = copies.astype(jnp.float32)
    weights_new = weights + mixing_rate * (copies_mixed.astype(jnp.float32) - copy_value) - step_rate * tracker.astype(jnp.float32)
    param_update = jax.vmap(compress)(row_picks[:, 0], weights_new - copy_value)
    copies_new = (copy_value + param_update).astype(jnp.bfloat16)
    mixed_new = (copies_mixed.astype(jnp.float32) + gossip_mix(param_update)).astype(jnp.bfloat16)

    def one_replica(packed):
        return replica_grad(packed[0], packed[1], packed[2], packed[3], key_weight, value_weight)
    grad_new = lax.map(one_replica, (weights_new, tokens, image_ids, out_grad))
    tracker_copy_value = tracker_copy.astype(jnp.float32)
    tracker_new = (tracker.astype(jnp.float32) + mixing_rate * (tracker_mixed.astype(jnp.float32) - tracker_copy_value) + grad_new.astype(jnp.float32) - grad_prev.astype(jnp.float32)).astype(jnp.bfloat16)
    tracker_update = jax.vmap(compress)(row_picks[:, 1], tracker_new.astype(jnp.float32) - tracker_copy_value)
    tracker_copy_new = (tracker_copy_value + tracker_update).astype(jnp.bfloat16)
    tracker_mixed_new = (tracker_mixed.astype(jnp.float32) + gossip_mix(tracker_update)).astype(jnp.bfloat16)
    gap_value = mixed_new.astype(jnp.float32) - copies_new.astype(jnp.float32)
    consensus = jnp.sum(gap_value * gap_value) / (N_BLK * D * D)
    return (weights_new, copies_new, mixed_new, tracker_new, tracker_copy_new, tracker_mixed_new, grad_new, consensus)
```

```python
import functools

import jax
import jax.numpy as jnp
from jax import lax
from jax.experimental import pallas as pl
from jax.experimental.pallas import tpu as pltpu
from jax.sharding import PartitionSpec as P

HD = 64
SEG_MOST = 197
TILE = 128

mixing_rate = 0.2
step_rate = 0.5

ANY = pl.BlockSpec(memory_space=pl.ANY)
VMEM = pl.BlockSpec(memory_space=pltpu.VMEM)
HBM = pl.BlockSpec(memory_space=pltpu.HBM)


def contract(left, right, left_dim, right_dim):
    return lax.dot_general(
        left, right, (((left_dim,), (right_dim,)), ((), ())), preferred_element_type=jnp.float32
    )


def one_hot(picks, total_rows):
    columns = lax.broadcasted_iota(jnp.int32, (picks.shape[0], total_rows), 1)
    return (picks[:, None] == columns).astype(jnp.bfloat16)


def picked_rows(picks, total_rows):
    rows = lax.broadcasted_iota(jnp.int32, (total_rows, picks.shape[0]), 0)
    return jnp.any(rows == picks[None, :], axis=1, keepdims=True)


def replica_picks(row_picks, offset):
    count = lax.axis_size("blk")
    rank = lax.rem(lax.axis_index("blk") + offset + count, count)
    return lax.dynamic_index_in_dim(row_picks, rank, 0, keepdims=False)


def mix_stream(pieces, row_picks, stream, total_rows):
    picks = jnp.concatenate([replica_picks(row_picks, o)[stream] for o in (-1, 0, 1)], axis=0)
    values = jnp.concatenate(pieces, axis=0)
    return contract(one_hot(picks, total_rows), values, 0, 0) / 3.0


def gossip_kernel(
    blk_count, tp_count, values, part, lower, upper, total, slots, send_sem, recv_sem, part_sems
):
    blk, tp = lax.axis_index("blk"), lax.axis_index("tp")
    count = blk_count * tp_count
    me = blk * tp_count + tp
    mesh_type = pl.DeviceIdType.MESH
    barrier = pltpu.get_barrier_semaphore()

    def device(distance):
        flat = lax.rem(me + distance, count)
        return (flat // tp_count, lax.rem(flat, tp_count))

    def greet(distance, carry):
        pl.semaphore_signal(barrier, inc=1, device_id=device(distance), device_id_type=mesh_type)
        return carry

    lax.fori_loop(1, count, greet, 0)
    pl.semaphore_wait(barrier, count - 1)
    after = lax.rem(blk + 1, blk_count)
    before = lax.rem(blk + blk_count - 1, blk_count)
    up = pltpu.make_async_remote_copy(
        values, lower, send_sem.at[0], recv_sem.at[0], device_id=(after, tp), device_id_type=mesh_type
    )
    down = pltpu.make_async_remote_copy(
        values, upper, send_sem.at[1], recv_sem.at[1], device_id=(before, tp), device_id_type=mesh_type
    )
    up.start()
    down.start()

    def send(distance, carry):
        pltpu.make_async_remote_copy(
            part,
            slots.at[distance - 1],
            part_sems.at[0],
            part_sems.at[1],
            device_id=device(distance),
            device_id_type=mesh_type,
        ).start()
        return carry

    lax.fori_loop(1, count, send, 0)
    pltpu.make_async_copy(slots, slots, part_sems.at[1]).wait()
    pltpu.make_async_copy(slots, slots, part_sems.at[0]).wait()
    total[...] = jnp.sum(slots[...], axis=0) + part[...]
    up.wait()
    down.wait()


def gossip(values, part):
    blk_count, tp_count = lax.axis_size("blk"), lax.axis_size("tp")
    same = jax.ShapeDtypeStruct(values.shape, values.dtype)
    return pl.pallas_call(
        functools.partial(gossip_kernel, blk_count, tp_count),
        out_shape=(same, same, jax.ShapeDtypeStruct(part.shape, part.dtype)),
        in_specs=[VMEM, VMEM],
        out_specs=(VMEM, VMEM, VMEM),
        scratch_shapes=[
            pltpu.VMEM((blk_count * tp_count - 1,) + part.shape, part.dtype),
            pltpu.SemaphoreType.DMA((2,)),
            pltpu.SemaphoreType.DMA((2,)),
            pltpu.SemaphoreType.DMA((2,)),
        ],
        compiler_params=pltpu.CompilerParams(collective_id=0, has_side_effects=True),
        cost_estimate=pl.CostEstimate(flops=10000, bytes_accessed=10000000, transcendentals=0),
    )(values, part)


def attend(lows, total_rows, qs, ks, vs, og, qg, ids_col, ids_row, bias):
    width = qs.shape[1]
    pair = 2 * HD
    lane = lax.broadcasted_iota(jnp.int32, (1, pair), 1)
    first = jnp.where(lane < HD, 1.0, 0.0).astype(jnp.bfloat16)
    second = jnp.where(lane < HD, 0.0, 1.0).astype(jnp.bfloat16)
    reach = SEG_MOST - 1
    for low in lows:
        start = max(0, (low - reach) // TILE * TILE)
        end = min(total_rows, -(-(low + TILE + reach) // TILE) * TILE)
        span = end - start
        same = ids_col[low : low + TILE, :] == ids_row[:, start:end]
        tile_bias = jnp.where(same, 0.0, -1e30)
        bias[:TILE, :span] = tile_bias
        bias[TILE:, :span] = tile_bias

        @pl.loop(0, width // pair, unroll=2 if width // pair % 2 == 0 else 1)
        def _(index):
            columns = pl.ds(pl.multiple_of(index * pair, pair), pair)
            query = qs[low : low + TILE, columns]
            outer = og[low : low + TILE, columns]
            keyed = ks[start:end, columns]
            valued = vs[start:end, columns]
            queries = jnp.concatenate([query * first, query * second], axis=0)
            outers = jnp.concatenate([outer * first, outer * second], axis=0)
            scores = contract(queries, keyed, 1, 1) + bias[:, :span]
            out_proj = contract(outers, valued, 1, 1)
            exponent = jnp.exp(scores - jnp.max(scores, axis=-1, keepdims=True))
            inverse = 1.0 / jnp.sum(exponent, axis=-1, keepdims=True)
            centre = jnp.sum(exponent * out_proj, axis=-1, keepdims=True) * inverse
            score_grad = (exponent * ((out_proj - centre) * (inverse * HD ** (-0.5)))).astype(
                jnp.bfloat16
            )
            both = jnp.dot(score_grad, keyed, preferred_element_type=jnp.float32)
            qg[low : low + TILE, columns] = jnp.where(lane < HD, both[:TILE], both[TILE:]).astype(
                jnp.bfloat16
            )


def project(start, steps, tok, qw, kw, vw, qs, ks, vs, proj):
    @pl.loop(0, steps)
    def _(step):
        rows = pl.ds(pl.multiple_of(start + step * proj, proj), proj)
        block = tok[rows, :]
        query = jnp.dot(block, qw[...], preferred_element_type=jnp.float32).astype(jnp.bfloat16)
        qs[rows, :] = (query.astype(jnp.float32) * HD ** (-0.5)).astype(jnp.bfloat16)
        ks[rows, :] = jnp.dot(block, kw[...], preferred_element_type=jnp.float32).astype(jnp.bfloat16)
        vs[rows, :] = jnp.dot(block, vw[...], preferred_element_type=jnp.float32).astype(jnp.bfloat16)


def piece_rows(index, rank, local, count):
    start = lax.rem(rank - index + count, count) * local
    return pl.ds(pl.multiple_of(start, local), local)


def span_limit(total_rows):
    return min(total_rows, TILE + 2 * (-(-(SEG_MOST - 1) // TILE) * TILE))


def gradient_kernel(count, *refs):
    pieces = refs[:count]
    (query_w, key_w, value_w, out_grad, ids_col, ids_row, picks_row, picks_col) = refs[count : count + 8]
    fields = refs[count + 8 : count + 12]
    grad_out, tracker_out, copy_out, kept = refs[count + 12 : count + 16]
    scratch = refs[count + 16 :]
    tok, qw, kw, vw, og, tr, tm, tc, gp, qs, ks, vs, qg, upd, bias, go, to, co, tok_sems, sems, out_sems = scratch
    total_rows, model_width = tok.shape
    rank = lax.axis_index("tp")

    loads = []
    for shift in range(count):
        where = piece_rows(shift, rank, pieces[0].shape[0], count)
        loads.append(pltpu.make_async_copy(pieces[shift], tok.at[where], tok_sems.at[shift]))
    sources = (query_w, key_w, value_w, out_grad) + fields
    for index, (source, target) in enumerate(zip(sources, (qw, kw, vw, og, tr, tm, tc, gp))):
        loads.append(pltpu.make_async_copy(source, target, sems.at[index]))
    for load in loads:
        load.start()
    for load in loads[: count + 4]:
        load.wait()

    project(0, total_rows // 256, tok, qw, kw, vw, qs, ks, vs, 256)
    attend(range(0, total_rows, TILE), total_rows, qs, ks, vs, og, qg, ids_col, ids_row, bias)

    for load in loads[count + 4 :]:
        load.wait()

    @pl.loop(0, model_width // TILE)
    def _(step):
        base = pl.multiple_of(step * TILE, TILE)
        rows = pl.ds(base, TILE)
        product = contract(tok[:, rows], qg[...], 0, 0)
        grad = (product * model_width ** (-0.5)).astype(jnp.bfloat16)
        copy = tc[rows, :].astype(jnp.float32)
        new = (
            tr[rows, :].astype(jnp.float32)
            + mixing_rate * (tm[rows, :].astype(jnp.float32) - copy)
            + grad.astype(jnp.float32)
            - gp[rows, :].astype(jnp.float32)
        ).astype(jnp.bfloat16)
        change = new.astype(jnp.float32) - copy
        index = lax.broadcasted_iota(jnp.int32, (TILE, picks_row.shape[1]), 0) + base
        hits = jnp.where(index == picks_row[...], 1.0, 0.0)
        picked = jnp.max(hits, axis=1, keepdims=True)
        go[rows, :] = grad
        to[rows, :] = new
        co[rows, :] = (copy + change * picked).astype(jnp.bfloat16)
        upd[rows, :] = change.astype(jnp.bfloat16)
        for slot, (source, target) in enumerate(((go, grad_out), (to, tracker_out), (co, copy_out))):
            pltpu.make_async_copy(source.at[rows], target.at[rows], out_sems.at[slot]).start()

    columns = lax.broadcasted_iota(jnp.int32, (picks_col.shape[0], model_width), 1)
    matrix = jnp.where(picks_col[...] == columns, 1.0, 0.0).astype(jnp.bfloat16)
    kept[...] = jnp.dot(matrix, upd[...], preferred_element_type=jnp.float32).astype(jnp.bfloat16)
    for slot, (source, target) in enumerate(((go, grad_out), (to, tracker_out), (co, copy_out))):
        pltpu.make_async_copy(source, target, out_sems.at[slot]).wait()


def gradient_stage(pieces, query_weight, key_weight, value_weight, out_grad, image_row, picks, fields):
    count = len(pieces)
    model_width = pieces[0].shape[1]
    total_rows = out_grad.shape[0]
    width = query_weight.shape[1]
    bf16 = jnp.bfloat16
    field = jax.ShapeDtypeStruct((model_width, width), bf16)
    weight = pltpu.VMEM((model_width, width), bf16)
    row_block = pltpu.VMEM((total_rows, width), bf16)
    return pl.pallas_call(
        functools.partial(gradient_kernel, count),
        out_shape=(field, field, field, jax.ShapeDtypeStruct((picks.shape[0], width), bf16)),
        in_specs=[ANY] * (count + 4) + [VMEM] * 4 + [ANY] * 4,
        out_specs=(ANY, ANY, ANY, VMEM),
        scratch_shapes=[pltpu.VMEM((total_rows, model_width), bf16)]
        + [weight] * 3
        + [row_block]
        + [weight] * 4
        + [row_block] * 4
        + [weight, pltpu.VMEM((2 * TILE, span_limit(total_rows)), jnp.float32)]
        + [weight] * 3
        + [
            pltpu.SemaphoreType.DMA((count,)),
            pltpu.SemaphoreType.DMA((8,)),
            pltpu.SemaphoreType.DMA((3,)),
        ],
        compiler_params=pltpu.CompilerParams(vmem_limit_bytes=56 * 2**20),
        cost_estimate=pl.CostEstimate(
            flops=8 * total_rows * model_width * width + 6 * total_rows * 640 * width,
            bytes_accessed=24 * model_width * width,
            transcendentals=total_rows * 640 * width // HD,
        ),
    )(
        *pieces,
        query_weight,
        key_weight,
        value_weight,
        out_grad,
        image_row.reshape(total_rows, 1),
        image_row.reshape(1, total_rows),
        picks.reshape(1, -1),
        picks.reshape(-1, 1),
        *fields,
    )


IMAGES = 6
PACK = 16
QUERY_ROWS = 224
KEY_ROWS = 256
MESH = pl.DeviceIdType.MESH


def token_chunks(local):
    edges = [0]
    for count in range(3, IMAGES):
        need = -(-(count * SEG_MOST - local) // 16) * 16
        edges.append(min(local, max(need, edges[-1])))
    edges.append(local)
    return list(zip(edges[:-1], edges[1:]))


def pick_column(picks, blk, stream):
    row = picks[blk, stream : stream + 1, :].astype(jnp.float32)
    size = row.shape[1]
    rows = lax.broadcasted_iota(jnp.int32, (size, size), 0)
    columns = lax.broadcasted_iota(jnp.int32, (size, size), 1)
    return jnp.sum(jnp.where(rows == columns, row, 0.0), axis=1, keepdims=True)


def hot_rows(column, total_rows):
    index = lax.broadcasted_iota(jnp.int32, (column.shape[0], total_rows), 1)
    return jnp.where(column == index.astype(jnp.float32), 1.0, 0.0).astype(jnp.bfloat16)


def picked_mask(picks, blk, stream, base, rows):
    row = picks[blk, stream : stream + 1, :]
    index = lax.broadcasted_iota(jnp.int32, (rows, row.shape[1]), 0) + base
    return jnp.max(jnp.where(index == row, 1.0, 0.0), axis=1, keepdims=True)


def window_start(low, ref, rows):
    return jnp.minimum(low // PACK, ref.shape[0] - rows // PACK)


def window(ref, block, rows, columns):
    parts = [ref[block + index, :, columns] for index in range(rows // PACK)]
    return jnp.concatenate(parts, axis=0)


def attend_image(slot, low, high, qs, ks, vs, og, qg):
    width = qs.shape[2]
    pair = 2 * HD
    lane = lax.broadcasted_iota(jnp.int32, (1, pair), 1)
    first = jnp.where(lane < HD, 1.0, 0.0).astype(jnp.bfloat16)
    second = jnp.where(lane < HD, 0.0, 1.0).astype(jnp.bfloat16)
    query_block = window_start(low, qs, QUERY_ROWS)
    key_block = window_start(low, qs, KEY_ROWS)
    position = lax.broadcasted_iota(jnp.int32, (1, KEY_ROWS), 1) + key_block * PACK
    bias = jnp.where((position >= low) & (position < high), 0.0, -1e30)
    row = lax.broadcasted_iota(jnp.int32, (QUERY_ROWS, pair), 0) + query_block * PACK
    inside = (row >= low) & (row < high)

    @pl.loop(0, width // pair, unroll=2)
    def _(index):
        columns = pl.ds(pl.multiple_of(index * pair, pair), pair)
        query = window(qs, query_block, QUERY_ROWS, columns)
        outer = window(og, query_block, QUERY_ROWS, columns)
        keyed = window(ks, key_block, KEY_ROWS, columns)
        valued = window(vs, key_block, KEY_ROWS, columns)
        queries = jnp.concatenate([query * first, query * second], axis=0)
        outers = jnp.concatenate([outer * first, outer * second], axis=0)
        scores = contract(queries, keyed, 1, 1) + bias
        out_proj = contract(outers, valued, 1, 1)
        exponent = jnp.exp(scores - jnp.max(scores, axis=-1, keepdims=True))
        inverse = 1.0 / jnp.sum(exponent, axis=-1, keepdims=True)
        centre = jnp.sum(exponent * out_proj, axis=-1, keepdims=True) * inverse
        score_grad = (exponent * ((out_proj - centre) * (inverse * HD ** (-0.5)))).astype(
            jnp.bfloat16
        )
        both = jnp.dot(score_grad, keyed, preferred_element_type=jnp.float32)
        merged = jnp.where(lane < HD, both[:QUERY_ROWS], both[QUERY_ROWS:])
        qg[slot, :, columns] = jnp.where(inside, merged, 0.0).astype(jnp.bfloat16)


def step_kernel(blk_count, chunks, *refs):
    (weights, copies, mixed, tracker, tracker_copy, tracker_mixed, grad_prev) = refs[:7]
    (tokens, ids, key_weight, value_weight, out_grad, row_picks) = refs[7:13]
    (w_out, copy_out, mix_out, grad_out, new_out, held_out, tm, values, spread, total) = refs[13:23]
    (wt, cp, mx, tr, tc, gp, kw, vw, og, qw, upd, tok, recv) = refs[23:36]
    (qs, ks, vs, qg, acc, base, id_row, picks, heard, hot, part, slots, group, other) = refs[36:50]
    (load_sem, send_tok, recv_tok, near, rise, fall, send_row, recv_row, sum_sem) = refs[50:]

    blk, tp = lax.axis_index("blk"), lax.axis_index("tp")
    planes = blk_count // 4
    plane = blk // 4
    blocks = tokens.shape[0]
    width = qs.shape[2]
    model_width = tok.shape[2]
    kept = row_picks.shape[2]
    partner = (blk, 1 - tp)
    after = (lax.rem(blk + 1, blk_count), tp)
    before = (lax.rem(blk + blk_count - 1, blk_count), tp)
    flip_two = (blk + 2 - 4 * (lax.rem(blk, 4) // 2), tp)
    flip_one = (blk + 1 - 2 * lax.rem(blk, 2), tp)
    below = (jnp.maximum(blk - 4, 0), tp)
    above = (jnp.minimum(blk + 4, blk_count - 1), tp)
    lowest = plane == 0
    highest = plane == planes - 1

    barrier = pltpu.get_barrier_semaphore()
    for device in (partner, flip_one, flip_two):
        pl.semaphore_signal(barrier, inc=1, device_id=device, device_id_type=MESH)

    def tell(lower, upper):
        @pl.when(jnp.logical_not(lowest))
        def _():
            pl.semaphore_signal(lower, inc=1, device_id=below, device_id_type=MESH)

        @pl.when(jnp.logical_not(highest))
        def _():
            pl.semaphore_signal(upper, inc=1, device_id=above, device_id_type=MESH)

    def hear(lower, upper):
        @pl.when(jnp.logical_not(highest))
        def _():
            pl.semaphore_wait(lower, 1)

        @pl.when(jnp.logical_not(lowest))
        def _():
            pl.semaphore_wait(upper, 1)

    tell(barrier, barrier)

    own = pl.ds(tp * blocks, blocks)
    far = pl.ds((1 - tp) * blocks, blocks)
    sources = (tokens, row_picks, ids, weights, copies, mixed, tracker)
    sources += (key_weight, value_weight, out_grad, tracker_copy, tracker_mixed, grad_prev)
    targets = (tok.at[own], picks, id_row, wt, cp, mx, tr, kw, vw, og, tc, tm, gp)
    loads = [
        pltpu.make_async_copy(source, target, load_sem.at[index])
        for index, (source, target) in enumerate(zip(sources, targets))
    ]
    for load in loads:
        load.start()
    loads[0].wait()
    pl.semaphore_wait(barrier, 5 - lowest.astype(jnp.int32) - highest.astype(jnp.int32))

    sends = []
    for index, (start, end) in enumerate(chunks):
        size = end - start
        first = blocks * tp + jnp.where(tp == 0, blocks - end, start)
        send = pltpu.make_async_remote_copy(
            tok.at[pl.ds(first, size)],
            recv.at[start:end],
            send_tok.at[index],
            recv_tok.at[index],
            device_id=partner,
            device_id_type=MESH,
        )
        send.start()
        sends.append(send)

    pl.semaphore_signal(near.at[0], inc=1, device_id=flip_two, device_id_type=MESH)

    for target in (qs, ks, vs, tok):
        target[far] = jnp.zeros((blocks,) + target.shape[1:], jnp.bfloat16)
    for load in loads[1:7]:
        load.wait()

    for stream, target in enumerate((hot, spread)):
        for index, shift in enumerate((blk_count - 1, 0, 1)):
            rank = lax.rem(blk + shift, blk_count)
            target[index * kept : (index + 1) * kept, :] = hot_rows(
                pick_column(picks, rank, stream), model_width
            )

    @pl.loop(0, model_width // TILE)
    def _(step):
        start = pl.multiple_of(step * TILE, TILE)
        rows = pl.ds(start, TILE)
        copy = cp[rows, :].astype(jnp.float32)
        new = (
            wt[rows, :]
            + mixing_rate * (mx[rows, :].astype(jnp.float32) - copy)
            - step_rate * tr[rows, :].astype(jnp.float32)
        )
        change = new - copy
        w_out[rows, :] = new
        query = (new * model_width ** (-0.5)).astype(jnp.bfloat16)
        qw[rows, :] = query * jnp.bfloat16(HD ** (-0.5))
        upd[rows, :] = change.astype(jnp.bfloat16)
        picked = picked_mask(picks, blk, 0, start, TILE)
        copy_out[rows, :] = jnp.where(picked > 0.5, copy + change, copy).astype(jnp.bfloat16)

    middle = slice(kept, 2 * kept)
    heard[middle, :] = jnp.dot(
        hot[middle, :], upd[...], preferred_element_type=jnp.float32
    ).astype(jnp.bfloat16)

    pl.semaphore_wait(near.at[0], 1)
    pl.semaphore_signal(near.at[1], inc=1, device_id=flip_one, device_id_type=MESH)

    edge = []
    for image in range(IMAGES + 1):
        edge.append(jnp.sum(jnp.where(id_row[...] < image, 1, 0)))

    def bounds(slot):
        low = jnp.where(tp == 0, edge[slot], edge[IMAGES - 1 - slot])
        high = jnp.where(tp == 0, edge[slot + 1], edge[IMAGES - slot])
        return low, high

    def project_block(block, rows):
        flat = block.reshape(-1, model_width)
        for target, weight in ((qs, qw), (ks, kw), (vs, vw)):
            result = jnp.dot(flat, weight[...], preferred_element_type=jnp.float32)
            target[rows] = result.astype(jnp.bfloat16).reshape(-1, PACK, width)

    loads[7].wait()
    loads[8].wait()

    @pl.loop(0, 2)
    def _(step):
        rows = pl.ds(tp * blocks + step * (blocks // 2), blocks // 2)
        project_block(tok[rows], rows)

    pl.semaphore_wait(near.at[1], 1)
    for stage in range(planes - 2):
        tell(fall.at[stage], rise.at[stage])
        if stage == 0:
            loads[9].wait()
            attend_image(0, *bounds(0), qs, ks, vs, og, qg)
        if stage == 1:
            attend_image(1, *bounds(1), qs, ks, vs, og, qg)
        hear(fall.at[stage], rise.at[stage])
    if planes < 3:
        loads[9].wait()
    for slot in range(min(2, planes - 2), 2):
        attend_image(slot, *bounds(slot), qs, ks, vs, og, qg)

    def swap(source, target, index):
        moves = []
        for way, (device, slot) in enumerate(((after, 0), (before, 2))):
            move = pltpu.make_async_remote_copy(
                source.at[middle],
                target.at[slot * kept : (slot + 1) * kept],
                send_row.at[2 * index + way],
                recv_row.at[2 * index + way],
                device_id=device,
                device_id_type=MESH,
            )
            move.start()
            moves.append(move)
        return moves

    param = swap(heard, heard, 0)

    def take(index):
        start, end = chunks[index]
        size = end - start
        sends[index].wait_recv()
        first = blocks * (1 - tp) + jnp.where(tp == 0, start, blocks - end)
        rows = pl.ds(first, size)
        block = recv[start:end]
        tok[rows] = block
        project_block(block, rows)

    take(0)
    attend_image(2, *bounds(2), qs, ks, vs, og, qg)

    for move in param:
        move.wait()
    part[...] = jnp.zeros_like(part)

    @pl.loop(0, model_width // TILE)
    def _(step):
        rows = pl.ds(pl.multiple_of(step * TILE, TILE), TILE)
        gain = contract(hot[:, rows], heard[...], 0, 0) / 3.0
        new = (mx[rows, :].astype(jnp.float32) + gain).astype(jnp.bfloat16)
        mix_out[rows, :] = new
        gap = new.astype(jnp.float32) - copy_out[rows, :].astype(jnp.float32)
        square = gap * gap
        folded = sum(square[:, at : at + 128] for at in range(0, width, 128))
        part[...] += jnp.sum(folded.reshape(TILE // 8, 8, 128), axis=0)

    slots[pl.ds(blk, 1)] = part[...][None]

    def share(distance):
        return pltpu.make_async_remote_copy(
            part,
            slots.at[blk],
            sum_sem.at[0],
            sum_sem.at[1],
            device_id=(lax.rem(blk + distance, blk_count), tp),
            device_id_type=MESH,
        )

    @pl.loop(1, blk_count)
    def _(distance):
        share(distance).start()

    for load in loads[10:]:
        load.wait()

    @pl.loop(0, model_width // TILE)
    def _(step):
        rows = pl.ds(pl.multiple_of(step * TILE, TILE), TILE)
        copy = tc[rows, :].astype(jnp.float32)
        base[rows, :] = (
            tr[rows, :].astype(jnp.float32)
            + mixing_rate * (tm[rows, :].astype(jnp.float32) - copy)
            - gp[rows, :].astype(jnp.float32)
        )

    take(1)
    attend_image(3, *bounds(3), qs, ks, vs, og, qg)

    def product(slots_used, rows):
        result = 0.0
        for slot in slots_used:
            block = window_start(bounds(slot)[0], tok, QUERY_ROWS)
            result += contract(window(tok, block, QUERY_ROWS, rows), qg[slot], 0, 0)
        return result

    @pl.loop(0, model_width // TILE)
    def _(step):
        rows = pl.ds(pl.multiple_of(step * TILE, TILE), TILE)
        acc[rows, :] = product(range(4), rows)

    most = pl.ds(0, blk_count - 1)
    for way in range(2):
        pltpu.make_async_copy(slots.at[most], slots.at[most], sum_sem.at[way]).wait()
    group[...] = jnp.sum(slots[...], axis=0)
    cross = pltpu.make_async_remote_copy(
        group, other, sum_sem.at[2], sum_sem.at[3], device_id=partner, device_id_type=MESH
    )
    cross.start()

    take(2)
    attend_image(4, *bounds(4), qs, ks, vs, og, qg)
    take(3)
    attend_image(5, *bounds(5), qs, ks, vs, og, qg)

    @pl.loop(0, model_width // TILE)
    def _(step):
        start = pl.multiple_of(step * TILE, TILE)
        rows = pl.ds(start, TILE)
        gradient = acc[rows, :] + product((4, 5), rows)
        grad = (gradient * model_width ** (-0.5)).astype(jnp.bfloat16)
        copy = tc[rows, :].astype(jnp.float32)
        new = (base[rows, :] + grad.astype(jnp.float32)).astype(jnp.bfloat16)
        change = new.astype(jnp.float32) - copy
        picked = picked_mask(picks, blk, 1, start, TILE)
        grad_out[rows, :] = grad
        new_out[rows, :] = new
        held_out[rows, :] = jnp.where(picked > 0.5, copy + change, copy).astype(jnp.bfloat16)
        upd[rows, :] = change.astype(jnp.bfloat16)

    values[middle, :] = jnp.dot(
        spread[middle, :], upd[...], preferred_element_type=jnp.float32
    ).astype(jnp.bfloat16)
    track = swap(values, values, 1)

    cross.wait()
    total[...] = group[...] + other[...]
    for send in sends:
        send.wait_send()
    for move in track:
        move.wait()


def finish_kernel(entries, *refs):
    sources, tm, values, spread, total = refs[:6], refs[6], refs[7], refs[8], refs[9]
    targets, mix_target, sum_target = refs[10:16], refs[16], refs[17]
    mixed, sems = refs[18:]
    model_width = tm.shape[0]
    moves = [
        pltpu.make_async_copy(source, target, sems.at[index])
        for index, (source, target) in enumerate(zip(sources, targets))
    ]
    for move in moves:
        move.start()

    @pl.loop(0, model_width // (2 * TILE))
    def _(step):
        rows = pl.ds(pl.multiple_of(step * 2 * TILE, 2 * TILE), 2 * TILE)
        gain = contract(spread[:, rows], values[...], 0, 0) / 3.0
        mixed[rows, :] = (tm[rows, :].astype(jnp.float32) + gain).astype(jnp.bfloat16)
        pltpu.make_async_copy(mixed.at[rows], mix_target.at[rows], sems.at[6]).start()

    sum_target[...] = jnp.full((1, 1), 0.0, jnp.float32) + jnp.sum(total[...]) / entries
    for move in moves:
        move.wait()
    pltpu.make_async_copy(mixed, mix_target, sems.at[6]).wait()


def fused_step(blk_count, arrays):
    (weights, _, _, _, _, _, _) = arrays[:7]
    (tokens, ids, key_weight, value_weight, out_grad, row_picks) = arrays[7:]
    model_width, width = weights.shape
    packed_tokens = tokens.reshape(-1, PACK, model_width)
    packed_grad = out_grad.reshape(-1, PACK, width)
    arrays = arrays[:7] + (packed_tokens, ids, key_weight, value_weight, packed_grad, row_picks)
    local = tokens.shape[0]
    total_rows = ids.shape[1]
    kept = row_picks.shape[2]
    chunks = [(start // PACK, end // PACK) for start, end in token_chunks(local)]
    planes = blk_count // 4
    bf16, f32 = jnp.bfloat16, jnp.float32
    field = pltpu.VMEM((model_width, width), bf16)
    wide = pltpu.VMEM((model_width, width), f32)
    rows = pltpu.VMEM((total_rows // PACK, PACK, width), bf16)
    lanes = pltpu.VMEM((8, 128), f32)
    heard = pltpu.VMEM((3 * kept, width), bf16)
    hot = pltpu.VMEM((3 * kept, model_width), bf16)
    dma = pltpu.SemaphoreType.DMA
    held = pl.pallas_call(
        functools.partial(step_kernel, blk_count, chunks),
        out_shape=(wide,) + (field,) * 6 + (heard, hot, lanes),
        in_specs=[HBM] * 13,
        out_specs=(VMEM,) * 10,
        scratch_shapes=[wide]
        + [field] * 7
        + [rows, field, field]
        + [pltpu.VMEM((count // PACK, PACK, model_width), bf16) for count in (total_rows, local)]
        + [rows] * 3
        + [pltpu.VMEM((IMAGES, QUERY_ROWS, width), bf16), wide, wide]
        + [pltpu.VMEM(ids.shape, jnp.int32), pltpu.VMEM(row_picks.shape, jnp.int32), heard, hot]
        + [lanes, pltpu.VMEM((blk_count, 8, 128), f32), lanes, lanes]
        + [dma((13,)), dma((len(chunks),)), dma((len(chunks),))]
        + [pltpu.SemaphoreType.REGULAR((2,))]
        + [pltpu.SemaphoreType.REGULAR((max(planes - 2, 1),))] * 2
        + [dma((4,)), dma((4,)), dma((4,))],
        compiler_params=pltpu.CompilerParams(
            collective_id=0, has_side_effects=True, vmem_limit_bytes=44 * 2**20
        ),
        cost_estimate=pl.CostEstimate(
            flops=8 * total_rows * model_width * width,
            bytes_accessed=24 * model_width * width,
            transcendentals=total_rows * 256 * width // HD,
        ),
    )(*arrays)
    flat = jax.ShapeDtypeStruct((model_width, width), bf16)
    entries = float(blk_count * model_width * model_width)
    outs = pl.pallas_call(
        functools.partial(finish_kernel, entries),
        out_shape=(jax.ShapeDtypeStruct((model_width, width), f32),)
        + (flat,) * 6
        + (jax.ShapeDtypeStruct((1, 1), f32),),
        in_specs=[VMEM] * 10,
        out_specs=(HBM,) * 7 + (VMEM,),
        scratch_shapes=[field, dma((7,))],
        compiler_params=pltpu.CompilerParams(vmem_limit_bytes=8 * 2**20),
        cost_estimate=pl.CostEstimate(
            flops=model_width * width * 400,
            bytes_accessed=16 * model_width * width,
            transcendentals=0,
        ),
    )(*held)
    weights_new, copies_new, mixed_new, grad_new, tracker_new, held_new, mixed_back, total = outs
    return (
        weights_new[None],
        copies_new[None],
        mixed_new[None],
        tracker_new[None],
        held_new[None],
        mixed_back[None],
        grad_new[None],
        total[0, 0],
    )


def fits_fused(blk_count, local, model_width, width):
    enough = (IMAGES - 1) * SEG_MOST <= 2 * local and 2 * SEG_MOST <= local <= 3 * SEG_MOST
    shapes = local % 256 == 0 and model_width % 256 == 0 and width % (4 * HD) == 0
    return enough and shapes and blk_count % 4 == 0 and blk_count >= 8


def device_step(
    weights,
    copies,
    copies_mixed,
    tracker,
    tracker_copy,
    tracker_mixed,
    grad_prev,
    tokens,
    image_ids,
    key_weight,
    value_weight,
    out_grad,
    row_picks,
):
    model_width = weights.shape[1]
    blk_count, tp_count = lax.axis_size("blk"), lax.axis_size("tp")
    local = tokens.shape[1]
    if tp_count == 2 and fits_fused(blk_count, local, *weights.shape[1:]):
        fields = (weights, copies, copies_mixed, tracker, tracker_copy, tracker_mixed, grad_prev)
        return fused_step(
            blk_count,
            tuple(field[0] for field in fields)
            + (tokens[0], image_ids, key_weight, value_weight, out_grad[0], row_picks),
        )
    pieces = [tokens[0]]
    for shift in range(1, tp_count):
        hop = [(i, (i + shift) % tp_count) for i in range(tp_count)]
        pieces.append(lax.ppermute(tokens[0], "tp", hop))
    own_picks = replica_picks(row_picks, 0)
    copy_value = copies[0].astype(jnp.float32)
    mixed_value = copies_mixed[0].astype(jnp.float32)
    weights_new = (
        weights[0]
        + mixing_rate * (mixed_value - copy_value)
        - step_rate * tracker[0].astype(jnp.float32)
    )
    query_weight = (weights_new * model_width ** (-0.5)).astype(jnp.bfloat16)
    update = weights_new - copy_value
    picked = picked_rows(own_picks[0], model_width)
    copies_new = jnp.where(picked, copy_value + update, copy_value).astype(jnp.bfloat16)
    kept = contract(
        one_hot(own_picks[0], model_width), update.astype(jnp.bfloat16), 1, 0
    ).astype(jnp.bfloat16)
    up = [(i, (i + 1) % blk_count) for i in range(blk_count)]
    down = [(j, i) for i, j in up]
    lower = lax.ppermute(kept, "blk", up)
    upper = lax.ppermute(kept, "blk", down)
    mixed_new = (
        mixed_value + mix_stream([lower, kept, upper], row_picks, 0, model_width)
    ).astype(jnp.bfloat16)
    gap = mixed_new.astype(jnp.float32) - copies_new.astype(jnp.float32)
    part = jnp.broadcast_to(jnp.sum(gap * gap)[None, None], (8, 128))

    part, query_weight = lax.optimization_barrier((part, query_weight))
    grad_new, tracker_new, tracker_copy_new, kept = gradient_stage(
        pieces,
        query_weight,
        key_weight,
        value_weight,
        out_grad[0],
        image_ids[0],
        own_picks[1],
        (tracker[0], tracker_mixed[0], tracker_copy[0], grad_prev[0]),
    )
    lower, upper, total = gossip(kept, part)
    tracker_mixed_new = (
        tracker_mixed[0].astype(jnp.float32)
        + mix_stream([lower, kept, upper], row_picks, 1, model_width)
    ).astype(jnp.bfloat16)
    entries = float(blk_count * model_width * model_width)
    return (
        weights_new[None],
        copies_new[None],
        mixed_new[None],
        tracker_new[None],
        tracker_copy_new[None],
        tracker_mixed_new[None],
        grad_new[None],
        total[0, 0] / entries,
    )


def solution(mesh):
    field = P("blk", None, "tp")
    return jax.shard_map(
        device_step,
        mesh=mesh,
        in_specs=(field,) * 7
        + (P("blk", "tp", None), P("blk", None), P(None, "tp"), P(None, "tp"), field, P()),
        out_specs=(field,) * 7 + (P(),),
        check_vma=False,
    )
```

```python
import functools

import jax
import jax.numpy as jnp
from jax import lax
from jax.experimental import pallas as pl
from jax.experimental.pallas import tpu as pltpu
from jax.sharding import PartitionSpec as P

HD = 64
SEG_MOST = 197
TILE = 128

mixing_rate = 0.2
step_rate = 0.5

ANY = pl.BlockSpec(memory_space=pl.ANY)
VMEM = pl.BlockSpec(memory_space=pltpu.VMEM)
HBM = pl.BlockSpec(memory_space=pltpu.HBM)


def contract(left, right, left_dim, right_dim):
    return lax.dot_general(
        left, right, (((left_dim,), (right_dim,)), ((), ())), preferred_element_type=jnp.float32
    )


def one_hot(picks, total_rows):
    columns = lax.broadcasted_iota(jnp.int32, (picks.shape[0], total_rows), 1)
    return (picks[:, None] == columns).astype(jnp.bfloat16)


def picked_rows(picks, total_rows):
    rows = lax.broadcasted_iota(jnp.int32, (total_rows, picks.shape[0]), 0)
    return jnp.any(rows == picks[None, :], axis=1, keepdims=True)


def replica_picks(row_picks, offset):
    count = lax.axis_size("blk")
    rank = lax.rem(lax.axis_index("blk") + offset + count, count)
    return lax.dynamic_index_in_dim(row_picks, rank, 0, keepdims=False)


def mix_stream(pieces, row_picks, stream, total_rows):
    picks = jnp.concatenate([replica_picks(row_picks, o)[stream] for o in (-1, 0, 1)], axis=0)
    values = jnp.concatenate(pieces, axis=0)
    return contract(one_hot(picks, total_rows), values, 0, 0) / 3.0


def gossip_kernel(
    blk_count, tp_count, values, part, lower, upper, total, slots, send_sem, recv_sem, part_sems
):
    blk, tp = lax.axis_index("blk"), lax.axis_index("tp")
    count = blk_count * tp_count
    me = blk * tp_count + tp
    mesh_type = pl.DeviceIdType.MESH
    barrier = pltpu.get_barrier_semaphore()

    def device(distance):
        flat = lax.rem(me + distance, count)
        return (flat // tp_count, lax.rem(flat, tp_count))

    def greet(distance, carry):
        pl.semaphore_signal(barrier, inc=1, device_id=device(distance), device_id_type=mesh_type)
        return carry

    lax.fori_loop(1, count, greet, 0)
    pl.semaphore_wait(barrier, count - 1)
    after = lax.rem(blk + 1, blk_count)
    before = lax.rem(blk + blk_count - 1, blk_count)
    up = pltpu.make_async_remote_copy(
        values, lower, send_sem.at[0], recv_sem.at[0], device_id=(after, tp), device_id_type=mesh_type
    )
    down = pltpu.make_async_remote_copy(
        values, upper, send_sem.at[1], recv_sem.at[1], device_id=(before, tp), device_id_type=mesh_type
    )
    up.start()
    down.start()

    def send(distance, carry):
        pltpu.make_async_remote_copy(
            part,
            slots.at[distance - 1],
            part_sems.at[0],
            part_sems.at[1],
            device_id=device(distance),
            device_id_type=mesh_type,
        ).start()
        return carry

    lax.fori_loop(1, count, send, 0)
    pltpu.make_async_copy(slots, slots, part_sems.at[1]).wait()
    pltpu.make_async_copy(slots, slots, part_sems.at[0]).wait()
    total[...] = jnp.sum(slots[...], axis=0) + part[...]
    up.wait()
    down.wait()


def gossip(values, part):
    blk_count, tp_count = lax.axis_size("blk"), lax.axis_size("tp")
    same = jax.ShapeDtypeStruct(values.shape, values.dtype)
    return pl.pallas_call(
        functools.partial(gossip_kernel, blk_count, tp_count),
        out_shape=(same, same, jax.ShapeDtypeStruct(part.shape, part.dtype)),
        in_specs=[VMEM, VMEM],
        out_specs=(VMEM, VMEM, VMEM),
        scratch_shapes=[
            pltpu.VMEM((blk_count * tp_count - 1,) + part.shape, part.dtype),
            pltpu.SemaphoreType.DMA((2,)),
            pltpu.SemaphoreType.DMA((2,)),
            pltpu.SemaphoreType.DMA((2,)),
        ],
        compiler_params=pltpu.CompilerParams(collective_id=0, has_side_effects=True),
        cost_estimate=pl.CostEstimate(flops=10000, bytes_accessed=10000000, transcendentals=0),
    )(values, part)


def attend(lows, total_rows, qs, ks, vs, og, qg, ids_col, ids_row, bias):
    width = qs.shape[1]
    pair = 2 * HD
    lane = lax.broadcasted_iota(jnp.int32, (1, pair), 1)
    first = jnp.where(lane < HD, 1.0, 0.0).astype(jnp.bfloat16)
    second = jnp.where(lane < HD, 0.0, 1.0).astype(jnp.bfloat16)
    reach = SEG_MOST - 1
    for low in lows:
        start = max(0, (low - reach) // TILE * TILE)
        end = min(total_rows, -(-(low + TILE + reach) // TILE) * TILE)
        span = end - start
        same = ids_col[low : low + TILE, :] == ids_row[:, start:end]
        tile_bias = jnp.where(same, 0.0, -1e30)
        bias[:TILE, :span] = tile_bias
        bias[TILE:, :span] = tile_bias

        @pl.loop(0, width // pair, unroll=2 if width // pair % 2 == 0 else 1)
        def _(index):
            columns = pl.ds(pl.multiple_of(index * pair, pair), pair)
            query = qs[low : low + TILE, columns]
            outer = og[low : low + TILE, columns]
            keyed = ks[start:end, columns]
            valued = vs[start:end, columns]
            queries = jnp.concatenate([query * first, query * second], axis=0)
            outers = jnp.concatenate([outer * first, outer * second], axis=0)
            scores = contract(queries, keyed, 1, 1) + bias[:, :span]
            out_proj = contract(outers, valued, 1, 1)
            exponent = jnp.exp(scores - jnp.max(scores, axis=-1, keepdims=True))
            inverse = 1.0 / jnp.sum(exponent, axis=-1, keepdims=True)
            centre = jnp.sum(exponent * out_proj, axis=-1, keepdims=True) * inverse
            score_grad = (exponent * ((out_proj - centre) * (inverse * HD ** (-0.5)))).astype(
                jnp.bfloat16
            )
            both = jnp.dot(score_grad, keyed, preferred_element_type=jnp.float32)
            qg[low : low + TILE, columns] = jnp.where(lane < HD, both[:TILE], both[TILE:]).astype(
                jnp.bfloat16
            )


def project(start, steps, tok, qw, kw, vw, qs, ks, vs, proj):
    @pl.loop(0, steps)
    def _(step):
        rows = pl.ds(pl.multiple_of(start + step * proj, proj), proj)
        block = tok[rows, :]
        query = jnp.dot(block, qw[...], preferred_element_type=jnp.float32).astype(jnp.bfloat16)
        qs[rows, :] = (query.astype(jnp.float32) * HD ** (-0.5)).astype(jnp.bfloat16)
        ks[rows, :] = jnp.dot(block, kw[...], preferred_element_type=jnp.float32).astype(jnp.bfloat16)
        vs[rows, :] = jnp.dot(block, vw[...], preferred_element_type=jnp.float32).astype(jnp.bfloat16)


def piece_rows(index, rank, local, count):
    start = lax.rem(rank - index + count, count) * local
    return pl.ds(pl.multiple_of(start, local), local)


def span_limit(total_rows):
    return min(total_rows, TILE + 2 * (-(-(SEG_MOST - 1) // TILE) * TILE))


def gradient_kernel(count, *refs):
    pieces = refs[:count]
    (query_w, key_w, value_w, out_grad, ids_col, ids_row, picks_row, picks_col) = refs[count : count + 8]
    fields = refs[count + 8 : count + 12]
    grad_out, tracker_out, copy_out, kept = refs[count + 12 : count + 16]
    scratch = refs[count + 16 :]
    tok, qw, kw, vw, og, tr, tm, tc, gp, qs, ks, vs, qg, upd, bias, go, to, co, tok_sems, sems, out_sems = scratch
    total_rows, model_width = tok.shape
    rank = lax.axis_index("tp")

    loads = []
    for shift in range(count):
        where = piece_rows(shift, rank, pieces[0].shape[0], count)
        loads.append(pltpu.make_async_copy(pieces[shift], tok.at[where], tok_sems.at[shift]))
    sources = (query_w, key_w, value_w, out_grad) + fields
    for index, (source, target) in enumerate(zip(sources, (qw, kw, vw, og, tr, tm, tc, gp))):
        loads.append(pltpu.make_async_copy(source, target, sems.at[index]))
    for load in loads:
        load.start()
    for load in loads[: count + 4]:
        load.wait()

    project(0, total_rows // 256, tok, qw, kw, vw, qs, ks, vs, 256)
    attend(range(0, total_rows, TILE), total_rows, qs, ks, vs, og, qg, ids_col, ids_row, bias)

    for load in loads[count + 4 :]:
        load.wait()

    @pl.loop(0, model_width // TILE)
    def _(step):
        base = pl.multiple_of(step * TILE, TILE)
        rows = pl.ds(base, TILE)
        product = contract(tok[:, rows], qg[...], 0, 0)
        grad = (product * model_width ** (-0.5)).astype(jnp.bfloat16)
        copy = tc[rows, :].astype(jnp.float32)
        new = (
            tr[rows, :].astype(jnp.float32)
            + mixing_rate * (tm[rows, :].astype(jnp.float32) - copy)
            + grad.astype(jnp.float32)
            - gp[rows, :].astype(jnp.float32)
        ).astype(jnp.bfloat16)
        change = new.astype(jnp.float32) - copy
        index = lax.broadcasted_iota(jnp.int32, (TILE, picks_row.shape[1]), 0) + base
        hits = jnp.where(index == picks_row[...], 1.0, 0.0)
        picked = jnp.max(hits, axis=1, keepdims=True)
        go[rows, :] = grad
        to[rows, :] = new
        co[rows, :] = (copy + change * picked).astype(jnp.bfloat16)
        upd[rows, :] = change.astype(jnp.bfloat16)
        for slot, (source, target) in enumerate(((go, grad_out), (to, tracker_out), (co, copy_out))):
            pltpu.make_async_copy(source.at[rows], target.at[rows], out_sems.at[slot]).start()

    columns = lax.broadcasted_iota(jnp.int32, (picks_col.shape[0], model_width), 1)
    matrix = jnp.where(picks_col[...] == columns, 1.0, 0.0).astype(jnp.bfloat16)
    kept[...] = jnp.dot(matrix, upd[...], preferred_element_type=jnp.float32).astype(jnp.bfloat16)
    for slot, (source, target) in enumerate(((go, grad_out), (to, tracker_out), (co, copy_out))):
        pltpu.make_async_copy(source, target, out_sems.at[slot]).wait()


def gradient_stage(pieces, query_weight, key_weight, value_weight, out_grad, image_row, picks, fields):
    count = len(pieces)
    model_width = pieces[0].shape[1]
    total_rows = out_grad.shape[0]
    width = query_weight.shape[1]
    bf16 = jnp.bfloat16
    field = jax.ShapeDtypeStruct((model_width, width), bf16)
    weight = pltpu.VMEM((model_width, width), bf16)
    row_block = pltpu.VMEM((total_rows, width), bf16)
    return pl.pallas_call(
        functools.partial(gradient_kernel, count),
        out_shape=(field, field, field, jax.ShapeDtypeStruct((picks.shape[0], width), bf16)),
        in_specs=[ANY] * (count + 4) + [VMEM] * 4 + [ANY] * 4,
        out_specs=(ANY, ANY, ANY, VMEM),
        scratch_shapes=[pltpu.VMEM((total_rows, model_width), bf16)]
        + [weight] * 3
        + [row_block]
        + [weight] * 4
        + [row_block] * 4
        + [weight, pltpu.VMEM((2 * TILE, span_limit(total_rows)), jnp.float32)]
        + [weight] * 3
        + [
            pltpu.SemaphoreType.DMA((count,)),
            pltpu.SemaphoreType.DMA((8,)),
            pltpu.SemaphoreType.DMA((3,)),
        ],
        compiler_params=pltpu.CompilerParams(vmem_limit_bytes=56 * 2**20),
        cost_estimate=pl.CostEstimate(
            flops=8 * total_rows * model_width * width + 6 * total_rows * 640 * width,
            bytes_accessed=24 * model_width * width,
            transcendentals=total_rows * 640 * width // HD,
        ),
    )(
        *pieces,
        query_weight,
        key_weight,
        value_weight,
        out_grad,
        image_row.reshape(total_rows, 1),
        image_row.reshape(1, total_rows),
        picks.reshape(1, -1),
        picks.reshape(-1, 1),
        *fields,
    )


IMAGES = 6
PACK = 16
WIDE = 256
QUERY_ROWS = 224
KEY_ROWS = 256
MESH = pl.DeviceIdType.MESH


def token_chunks(local):
    edges = [0]
    for count in range(3, IMAGES):
        need = -(-(count * SEG_MOST - local) // 16) * 16
        edges.append(min(local, max(need, edges[-1])))
    edges.insert(-1, edges[-1] - 2 * PACK)
    edges.append(local)
    return list(zip(edges[:-1], edges[1:]))


def pick_column(picks, blk, stream):
    row = picks[blk, stream : stream + 1, :].astype(jnp.float32)
    size = row.shape[1]
    rows = lax.broadcasted_iota(jnp.int32, (size, size), 0)
    columns = lax.broadcasted_iota(jnp.int32, (size, size), 1)
    return jnp.sum(jnp.where(rows == columns, row, 0.0), axis=1, keepdims=True)


def hot_rows(column, total_rows):
    index = lax.broadcasted_iota(jnp.int32, (column.shape[0], total_rows), 1)
    return jnp.where(column == index.astype(jnp.float32), 1.0, 0.0).astype(jnp.bfloat16)


def picked_mask(picks, blk, stream, base, rows):
    row = picks[blk, stream : stream + 1, :]
    index = lax.broadcasted_iota(jnp.int32, (rows, row.shape[1]), 0) + base
    return jnp.max(jnp.where(index == row, 1.0, 0.0), axis=1, keepdims=True)


def window_start(low, ref, rows):
    return jnp.minimum(low // PACK, ref.shape[0] - rows // PACK)


def window(ref, block, rows, columns):
    parts = [ref[block + index, :, columns] for index in range(rows // PACK)]
    return jnp.concatenate(parts, axis=0)


def attend_image(slot, low, high, qs, ks, vs, og, qg):
    width = qs.shape[2]
    pair = 2 * HD
    lane = lax.broadcasted_iota(jnp.int32, (1, pair), 1)
    first = jnp.where(lane < HD, 1.0, 0.0).astype(jnp.bfloat16)
    second = jnp.where(lane < HD, 0.0, 1.0).astype(jnp.bfloat16)
    scale = jnp.bfloat16(HD ** (-0.5))
    first_scaled, second_scaled = first * scale, second * scale
    query_block = window_start(low, qs, QUERY_ROWS)
    key_block = window_start(low, qs, KEY_ROWS)
    position = lax.broadcasted_iota(jnp.int32, (1, KEY_ROWS), 1) + key_block * PACK
    bias = jnp.where((position >= low) & (position < high), 0.0, -1e30)
    row = lax.broadcasted_iota(jnp.int32, (QUERY_ROWS, pair), 0) + query_block * PACK
    inside = (row >= low) & (row < high)

    @pl.loop(0, width // pair, unroll=4)
    def _(index):
        columns = pl.ds(pl.multiple_of(index * pair, pair), pair)
        query = window(qs, query_block, QUERY_ROWS, columns)
        outer = window(og, query_block, QUERY_ROWS, columns)
        keyed = window(ks, key_block, KEY_ROWS, columns)
        valued = window(vs, key_block, KEY_ROWS, columns)
        queries = jnp.concatenate([query * first, query * second], axis=0)
        outers = jnp.concatenate([outer * first_scaled, outer * second_scaled], axis=0)
        scores = contract(queries, keyed, 1, 1) + bias
        out_proj = contract(outers, valued, 1, 1)
        exponent = jnp.exp(scores - jnp.max(scores, axis=-1, keepdims=True))
        inverse = 1.0 / jnp.sum(exponent, axis=-1, keepdims=True)
        centre = jnp.sum(exponent * out_proj, axis=-1, keepdims=True) * inverse
        score_grad = (exponent * ((out_proj - centre) * inverse)).astype(jnp.bfloat16)
        both = jnp.dot(score_grad, keyed, preferred_element_type=jnp.float32)
        merged = jnp.where(lane < HD, both[:QUERY_ROWS], both[QUERY_ROWS:])
        qg[slot, :, columns] = jnp.where(inside, merged, 0.0).astype(jnp.bfloat16)


def step_kernel(blk_count, chunks, *refs):
    (weights, copies, mixed, tracker, tracker_copy, tracker_mixed, grad_prev) = refs[:7]
    (tokens, ids, key_weight, value_weight, out_grad, row_picks) = refs[7:13]
    (w_out, copy_out, mix_out, grad_out, new_out, held_out, tm, values, spread, total) = refs[13:23]
    (wt, cp, mx, tr, tc, gp, kw, vw, og, qw, upd, tok, recv) = refs[23:36]
    (qs, ks, vs, qg, acc, base, id_row, picks, heard, hot, part, slots, group, other) = refs[36:50]
    selected, base_rows, copy_rows, grad_rows = refs[50:54]
    (load_sem, send_tok, recv_tok, near, rise, fall, send_row, recv_row, sum_sem) = refs[54:]

    blk, tp = lax.axis_index("blk"), lax.axis_index("tp")
    planes = blk_count // 4
    plane = blk // 4
    blocks = tokens.shape[0]
    width = qs.shape[2]
    model_width = tok.shape[2]
    kept = row_picks.shape[2]
    partner = (blk, 1 - tp)
    after = (lax.rem(blk + 1, blk_count), tp)
    before = (lax.rem(blk + blk_count - 1, blk_count), tp)
    flip_two = (blk + 2 - 4 * (lax.rem(blk, 4) // 2), tp)
    flip_one = (blk + 1 - 2 * lax.rem(blk, 2), tp)
    below = (jnp.maximum(blk - 4, 0), tp)
    above = (jnp.minimum(blk + 4, blk_count - 1), tp)
    lowest = plane == 0
    highest = plane == planes - 1

    barrier = pltpu.get_barrier_semaphore()
    for device in (partner, flip_one, flip_two):
        pl.semaphore_signal(barrier, inc=1, device_id=device, device_id_type=MESH)

    def tell(lower, upper):
        @pl.when(jnp.logical_not(lowest))
        def _():
            pl.semaphore_signal(lower, inc=1, device_id=below, device_id_type=MESH)

        @pl.when(jnp.logical_not(highest))
        def _():
            pl.semaphore_signal(upper, inc=1, device_id=above, device_id_type=MESH)

    def hear(lower, upper):
        @pl.when(jnp.logical_not(highest))
        def _():
            pl.semaphore_wait(lower, 1)

        @pl.when(jnp.logical_not(lowest))
        def _():
            pl.semaphore_wait(upper, 1)

    tell(barrier, barrier)

    own = pl.ds(tp * blocks, blocks)
    far = pl.ds((1 - tp) * blocks, blocks)
    sources = (tokens, row_picks, ids, weights, copies, mixed, tracker)
    sources += (key_weight, value_weight, out_grad, tracker_copy, tracker_mixed, grad_prev)
    targets = (tok.at[own], picks, id_row, wt, cp, mx, tr, kw, vw, og, tc, tm, gp)
    loads = [
        pltpu.make_async_copy(source, target, load_sem.at[index])
        for index, (source, target) in enumerate(zip(sources, targets))
    ]
    for load in loads:
        load.start()
    pl.semaphore_wait(barrier, 5 - lowest.astype(jnp.int32) - highest.astype(jnp.int32))

    sends = []
    for index, (start, end) in enumerate(chunks):
        size = end - start
        first = jnp.where(tp == 0, blocks - end, start)
        send = pltpu.make_async_remote_copy(
            tokens.at[pl.ds(first, size)],
            recv.at[start:end],
            send_tok.at[index],
            recv_tok.at[index],
            device_id=partner,
            device_id_type=MESH,
        )
        send.start()
        sends.append(send)

    pl.semaphore_signal(near.at[0], inc=1, device_id=flip_two, device_id_type=MESH)

    for target in (qs, ks, vs, tok, selected):
        target[far] = jnp.zeros((blocks,) + target.shape[1:], jnp.bfloat16)
    for load in loads[:7]:
        load.wait()

    for stream, target in enumerate((hot, spread)):
        for index, shift in enumerate((blk_count - 1, 0, 1)):
            rank = lax.rem(blk + shift, blk_count)
            target[index * kept : (index + 1) * kept, :] = hot_rows(
                pick_column(picks, rank, stream), model_width
            )

    @pl.loop(0, model_width // TILE)
    def _(step):
        start = pl.multiple_of(step * TILE, TILE)
        rows = pl.ds(start, TILE)
        copy = cp[rows, :].astype(jnp.float32)
        new = (
            wt[rows, :]
            + mixing_rate * (mx[rows, :].astype(jnp.float32) - copy)
            - step_rate * tr[rows, :].astype(jnp.float32)
        )
        change = new - copy
        w_out[rows, :] = new
        query = (new * model_width ** (-0.5)).astype(jnp.bfloat16)
        qw[rows, :] = query * jnp.bfloat16(HD ** (-0.5))
        upd[rows, :] = change.astype(jnp.bfloat16)
        picked = picked_mask(picks, blk, 0, start, TILE)
        copy_out[rows, :] = jnp.where(picked > 0.5, copy + change, copy).astype(jnp.bfloat16)

    middle = slice(kept, 2 * kept)
    heard[middle, :] = jnp.dot(
        hot[middle, :], upd[...], preferred_element_type=jnp.float32
    ).astype(jnp.bfloat16)

    pl.semaphore_wait(near.at[0], 1)
    pl.semaphore_signal(near.at[1], inc=1, device_id=flip_one, device_id_type=MESH)

    edge = []
    for image in range(IMAGES + 1):
        edge.append(jnp.sum(jnp.where(id_row[...] < image, 1, 0)))

    def bounds(slot):
        low = jnp.where(tp == 0, edge[slot], edge[IMAGES - 1 - slot])
        high = jnp.where(tp == 0, edge[slot + 1], edge[IMAGES - slot])
        return low, high

    def project_block(block, rows):
        flat = block.reshape(-1, model_width)
        for target, weight in ((qs, qw), (ks, kw), (vs, vw)):
            result = jnp.dot(flat, weight[...], preferred_element_type=jnp.float32)
            target[rows] = result.astype(jnp.bfloat16).reshape(-1, PACK, width)
        columns = contract(flat, spread[middle, :], 1, 1)
        selected[rows] = columns.astype(jnp.bfloat16).reshape(-1, PACK, kept)

    loads[7].wait()
    loads[8].wait()

    @pl.loop(0, 2)
    def _(step):
        rows = pl.ds(tp * blocks + step * (blocks // 2), blocks // 2)
        project_block(tok[rows], rows)

    pl.semaphore_wait(near.at[1], 1)
    for stage in range(planes - 2):
        tell(fall.at[stage], rise.at[stage])
        if stage == 0:
            loads[9].wait()
            attend_image(0, *bounds(0), qs, ks, vs, og, qg)
        if stage == 1:
            attend_image(1, *bounds(1), qs, ks, vs, og, qg)
        hear(fall.at[stage], rise.at[stage])
    if planes < 3:
        loads[9].wait()
    for slot in range(min(2, planes - 2), 2):
        attend_image(slot, *bounds(slot), qs, ks, vs, og, qg)

    def swap(source, target, index):
        moves = []
        for way, (device, slot) in enumerate(((after, 0), (before, 2))):
            move = pltpu.make_async_remote_copy(
                source.at[middle],
                target.at[slot * kept : (slot + 1) * kept],
                send_row.at[2 * index + way],
                recv_row.at[2 * index + way],
                device_id=device,
                device_id_type=MESH,
            )
            move.start()
            moves.append(move)
        return moves

    param = swap(heard, heard, 0)

    def take(index):
        start, end = chunks[index]
        size = end - start
        sends[index].wait_recv()
        first = blocks * (1 - tp) + jnp.where(tp == 0, start, blocks - end)
        rows = pl.ds(first, size)
        block = recv[start:end]
        tok[rows] = block
        project_block(block, rows)

    take(0)
    attend_image(2, *bounds(2), qs, ks, vs, og, qg)

    for load in loads[10:]:
        load.wait()

    @pl.loop(0, model_width // TILE)
    def _(step):
        rows = pl.ds(pl.multiple_of(step * TILE, TILE), TILE)
        copy = tc[rows, :].astype(jnp.float32)
        base[rows, :] = (
            tr[rows, :].astype(jnp.float32)
            + mixing_rate * (tm[rows, :].astype(jnp.float32) - copy)
            - gp[rows, :].astype(jnp.float32)
        )

    def rows_of(source):
        return jnp.dot(spread[middle, :], source[...], preferred_element_type=jnp.float32)

    copy_rows[...] = rows_of(tc)
    base_rows[...] = (
        rows_of(tr) + mixing_rate * (rows_of(tm) - copy_rows[...]) - rows_of(gp)
    )

    take(1)
    attend_image(3, *bounds(3), qs, ks, vs, og, qg)

    for move in param:
        move.wait()
    part[...] = jnp.zeros_like(part)

    @pl.loop(0, model_width // WIDE)
    def _(step):
        rows = pl.ds(pl.multiple_of(step * WIDE, WIDE), WIDE)
        gain = contract(hot[:, rows], heard[...], 0, 0) / 3.0
        new = (mx[rows, :].astype(jnp.float32) + gain).astype(jnp.bfloat16)
        mix_out[rows, :] = new
        gap = new.astype(jnp.float32) - copy_out[rows, :].astype(jnp.float32)
        square = gap * gap
        folded = sum(square[:, at : at + 128] for at in range(0, width, 128))
        part[...] += jnp.sum(folded.reshape(WIDE // 8, 8, 128), axis=0)

    slots[pl.ds(blk, 1)] = part[...][None]

    def share(distance):
        return pltpu.make_async_remote_copy(
            part,
            slots.at[blk],
            sum_sem.at[0],
            sum_sem.at[1],
            device_id=(lax.rem(blk + distance, blk_count), tp),
            device_id_type=MESH,
        )

    @pl.loop(1, blk_count)
    def _(distance):
        share(distance).start()


    def product(source, slots_used, columns):
        result = 0.0
        for slot in slots_used:
            block = window_start(bounds(slot)[0], source, QUERY_ROWS)
            result += contract(window(source, block, QUERY_ROWS, columns), qg[slot], 0, 0)
        return result

    grad_rows[...] = product(selected, range(4), slice(None))

    @pl.loop(0, model_width // WIDE)
    def _(step):
        rows = pl.ds(pl.multiple_of(step * WIDE, WIDE), WIDE)
        acc[rows, :] = product(tok, range(4), rows)

    take(2)
    take(3)
    attend_image(4, *bounds(4), qs, ks, vs, og, qg)
    take(4)
    attend_image(5, *bounds(5), qs, ks, vs, og, qg)

    gradient = grad_rows[...] + product(selected, (4, 5), slice(None))
    grad = (gradient * model_width ** (-0.5)).astype(jnp.bfloat16)
    new = (base_rows[...] + grad.astype(jnp.float32)).astype(jnp.bfloat16)
    values[middle, :] = (new.astype(jnp.float32) - copy_rows[...]).astype(jnp.bfloat16)
    track = swap(values, values, 1)

    most = pl.ds(0, blk_count - 1)
    for way in range(2):
        pltpu.make_async_copy(slots.at[most], slots.at[most], sum_sem.at[way]).wait()
    group[...] = jnp.sum(slots[...], axis=0)
    cross = pltpu.make_async_remote_copy(
        group, other, sum_sem.at[2], sum_sem.at[3], device_id=partner, device_id_type=MESH
    )
    cross.start()

    @pl.loop(0, model_width // WIDE)
    def _(step):
        start = pl.multiple_of(step * WIDE, WIDE)
        rows = pl.ds(start, WIDE)
        gradient = acc[rows, :] + product(tok, (4, 5), rows)
        grad = (gradient * model_width ** (-0.5)).astype(jnp.bfloat16)
        copy = tc[rows, :].astype(jnp.float32)
        new = (base[rows, :] + grad.astype(jnp.float32)).astype(jnp.bfloat16)
        change = new.astype(jnp.float32) - copy
        picked = picked_mask(picks, blk, 1, start, WIDE)
        grad_out[rows, :] = grad
        new_out[rows, :] = new
        held_out[rows, :] = jnp.where(picked > 0.5, copy + change, copy).astype(jnp.bfloat16)

    cross.wait()
    total[...] = group[...] + other[...]
    for send in sends:
        send.wait_send()
    for move in track:
        move.wait()


def finish_kernel(entries, *refs):
    sources, tm, values, spread, total = refs[:6], refs[6], refs[7], refs[8], refs[9]
    targets, mix_target, sum_target = refs[10:16], refs[16], refs[17]
    mixed, sems = refs[18:]
    model_width = tm.shape[0]
    moves = [
        pltpu.make_async_copy(source, target, sems.at[index])
        for index, (source, target) in enumerate(zip(sources, targets))
    ]
    for move in moves:
        move.start()

    @pl.loop(0, model_width // (2 * TILE))
    def _(step):
        rows = pl.ds(pl.multiple_of(step * 2 * TILE, 2 * TILE), 2 * TILE)
        gain = contract(spread[:, rows], values[...], 0, 0) / 3.0
        mixed[rows, :] = (tm[rows, :].astype(jnp.float32) + gain).astype(jnp.bfloat16)
        pltpu.make_async_copy(mixed.at[rows], mix_target.at[rows], sems.at[6]).start()

    sum_target[...] = jnp.full((1, 1), 0.0, jnp.float32) + jnp.sum(total[...]) / entries
    for move in moves:
        move.wait()
    pltpu.make_async_copy(mixed, mix_target, sems.at[6]).wait()


def fused_step(blk_count, arrays):
    (weights, _, _, _, _, _, _) = arrays[:7]
    (tokens, ids, key_weight, value_weight, out_grad, row_picks) = arrays[7:]
    model_width, width = weights.shape
    packed_tokens = tokens.reshape(-1, PACK, model_width)
    packed_grad = out_grad.reshape(-1, PACK, width)
    arrays = arrays[:7] + (packed_tokens, ids, key_weight, value_weight, packed_grad, row_picks)
    local = tokens.shape[0]
    total_rows = ids.shape[1]
    kept = row_picks.shape[2]
    chunks = [(start // PACK, end // PACK) for start, end in token_chunks(local)]
    planes = blk_count // 4
    bf16, f32 = jnp.bfloat16, jnp.float32
    field = pltpu.VMEM((model_width, width), bf16)
    wide = pltpu.VMEM((model_width, width), f32)
    rows = pltpu.VMEM((total_rows // PACK, PACK, width), bf16)
    lanes = pltpu.VMEM((8, 128), f32)
    heard = pltpu.VMEM((3 * kept, width), bf16)
    hot = pltpu.VMEM((3 * kept, model_width), bf16)
    dma = pltpu.SemaphoreType.DMA
    held = pl.pallas_call(
        functools.partial(step_kernel, blk_count, chunks),
        out_shape=(wide,) + (field,) * 6 + (heard, hot, lanes),
        in_specs=[HBM] * 13,
        out_specs=(VMEM,) * 10,
        scratch_shapes=[wide]
        + [field] * 7
        + [rows, field, field]
        + [pltpu.VMEM((count // PACK, PACK, model_width), bf16) for count in (total_rows, local)]
        + [rows] * 3
        + [pltpu.VMEM((IMAGES, QUERY_ROWS, width), bf16), wide, wide]
        + [pltpu.VMEM(ids.shape, jnp.int32), pltpu.VMEM(row_picks.shape, jnp.int32), heard, hot]
        + [lanes, pltpu.VMEM((blk_count, 8, 128), f32), lanes, lanes]
        + [pltpu.VMEM((total_rows // PACK, PACK, kept), bf16)]
        + [pltpu.VMEM((kept, width), f32)] * 3
        + [dma((13,)), dma((len(chunks),)), dma((len(chunks),))]
        + [pltpu.SemaphoreType.REGULAR((2,))]
        + [pltpu.SemaphoreType.REGULAR((max(planes - 2, 1),))] * 2
        + [dma((4,)), dma((4,)), dma((4,))],
        compiler_params=pltpu.CompilerParams(
            collective_id=0, has_side_effects=True, vmem_limit_bytes=44 * 2**20
        ),
        cost_estimate=pl.CostEstimate(
            flops=8 * total_rows * model_width * width,
            bytes_accessed=24 * model_width * width,
            transcendentals=total_rows * 256 * width // HD,
        ),
    )(*(pltpu.with_memory_space_constraint(array, pltpu.HBM) for array in arrays))
    flat = jax.ShapeDtypeStruct((model_width, width), bf16)
    entries = float(blk_count * model_width * model_width)
    outs = pl.pallas_call(
        functools.partial(finish_kernel, entries),
        out_shape=(jax.ShapeDtypeStruct((model_width, width), f32),)
        + (flat,) * 6
        + (jax.ShapeDtypeStruct((1, 1), f32),),
        in_specs=[VMEM] * 10,
        out_specs=(HBM,) * 7 + (VMEM,),
        scratch_shapes=[field, dma((7,))],
        compiler_params=pltpu.CompilerParams(vmem_limit_bytes=8 * 2**20),
        cost_estimate=pl.CostEstimate(
            flops=model_width * width * 400,
            bytes_accessed=16 * model_width * width,
            transcendentals=0,
        ),
    )(*held)
    weights_new, copies_new, mixed_new, grad_new, tracker_new, held_new, mixed_back, total = outs
    return (
        weights_new[None],
        copies_new[None],
        mixed_new[None],
        tracker_new[None],
        held_new[None],
        mixed_back[None],
        grad_new[None],
        total[0, 0],
    )


def fits_fused(blk_count, local, model_width, width):
    enough = (IMAGES - 1) * SEG_MOST <= 2 * local and 2 * SEG_MOST <= local <= 3 * SEG_MOST
    shapes = local % 256 == 0 and model_width % 256 == 0 and width % (4 * HD) == 0
    return enough and shapes and blk_count % 4 == 0 and blk_count >= 8


def device_step(
    weights,
    copies,
    copies_mixed,
    tracker,
    tracker_copy,
    tracker_mixed,
    grad_prev,
    tokens,
    image_ids,
    key_weight,
    value_weight,
    out_grad,
    row_picks,
):
    model_width = weights.shape[1]
    blk_count, tp_count = lax.axis_size("blk"), lax.axis_size("tp")
    local = tokens.shape[1]
    if tp_count == 2 and fits_fused(blk_count, local, *weights.shape[1:]):
        fields = (weights, copies, copies_mixed, tracker, tracker_copy, tracker_mixed, grad_prev)
        return fused_step(
            blk_count,
            tuple(field[0] for field in fields)
            + (tokens[0], image_ids, key_weight, value_weight, out_grad[0], row_picks),
        )
    pieces = [tokens[0]]
    for shift in range(1, tp_count):
        hop = [(i, (i + shift) % tp_count) for i in range(tp_count)]
        pieces.append(lax.ppermute(tokens[0], "tp", hop))
    own_picks = replica_picks(row_picks, 0)
    copy_value = copies[0].astype(jnp.float32)
    mixed_value = copies_mixed[0].astype(jnp.float32)
    weights_new = (
        weights[0]
        + mixing_rate * (mixed_value - copy_value)
        - step_rate * tracker[0].astype(jnp.float32)
    )
    query_weight = (weights_new * model_width ** (-0.5)).astype(jnp.bfloat16)
    update = weights_new - copy_value
    picked = picked_rows(own_picks[0], model_width)
    copies_new = jnp.where(picked, copy_value + update, copy_value).astype(jnp.bfloat16)
    kept = contract(
        one_hot(own_picks[0], model_width), update.astype(jnp.bfloat16), 1, 0
    ).astype(jnp.bfloat16)
    up = [(i, (i + 1) % blk_count) for i in range(blk_count)]
    down = [(j, i) for i, j in up]
    lower = lax.ppermute(kept, "blk", up)
    upper = lax.ppermute(kept, "blk", down)
    mixed_new = (
        mixed_value + mix_stream([lower, kept, upper], row_picks, 0, model_width)
    ).astype(jnp.bfloat16)
    gap = mixed_new.astype(jnp.float32) - copies_new.astype(jnp.float32)
    part = jnp.broadcast_to(jnp.sum(gap * gap)[None, None], (8, 128))

    part, query_weight = lax.optimization_barrier((part, query_weight))
    grad_new, tracker_new, tracker_copy_new, kept = gradient_stage(
        pieces,
        query_weight,
        key_weight,
        value_weight,
        out_grad[0],
        image_ids[0],
        own_picks[1],
        (tracker[0], tracker_mixed[0], tracker_copy[0], grad_prev[0]),
    )
    lower, upper, total = gossip(kept, part)
    tracker_mixed_new = (
        tracker_mixed[0].astype(jnp.float32)
        + mix_stream([lower, kept, upper], row_picks, 1, model_width)
    ).astype(jnp.bfloat16)
    entries = float(blk_count * model_width * model_width)
    return (
        weights_new[None],
        copies_new[None],
        mixed_new[None],
        tracker_new[None],
        tracker_copy_new[None],
        tracker_mixed_new[None],
        grad_new[None],
        total[0, 0] / entries,
    )


def solution(mesh):
    field = P("blk", None, "tp")
    return jax.shard_map(
        device_step,
        mesh=mesh,
        in_specs=(field,) * 7
        + (P("blk", "tp", None), P("blk", None), P(None, "tp"), P(None, "tp"), field, P()),
        out_specs=(field,) * 7 + (P(),),
        check_vma=False,
    )
```

```python
import functools

import jax
import jax.numpy as jnp
from jax import lax
from jax.experimental import pallas as pl
from jax.experimental.pallas import tpu as pltpu
from jax.sharding import PartitionSpec as P

HD = 64
SEG_MOST = 197
TILE = 128

mixing_rate = 0.2
step_rate = 0.5

ANY = pl.BlockSpec(memory_space=pl.ANY)
VMEM = pl.BlockSpec(memory_space=pltpu.VMEM)
HBM = pl.BlockSpec(memory_space=pltpu.HBM)


def contract(left, right, left_dim, right_dim):
    return lax.dot_general(
        left, right, (((left_dim,), (right_dim,)), ((), ())), preferred_element_type=jnp.float32
    )


def one_hot(picks, total_rows):
    columns = lax.broadcasted_iota(jnp.int32, (picks.shape[0], total_rows), 1)
    return (picks[:, None] == columns).astype(jnp.bfloat16)


def picked_rows(picks, total_rows):
    rows = lax.broadcasted_iota(jnp.int32, (total_rows, picks.shape[0]), 0)
    return jnp.any(rows == picks[None, :], axis=1, keepdims=True)


def replica_picks(row_picks, offset):
    count = lax.axis_size("blk")
    rank = lax.rem(lax.axis_index("blk") + offset + count, count)
    return lax.dynamic_index_in_dim(row_picks, rank, 0, keepdims=False)


def mix_stream(pieces, row_picks, stream, total_rows):
    picks = jnp.concatenate([replica_picks(row_picks, o)[stream] for o in (-1, 0, 1)], axis=0)
    values = jnp.concatenate(pieces, axis=0)
    return contract(one_hot(picks, total_rows), values, 0, 0) / 3.0


def gossip_kernel(
    blk_count, tp_count, values, part, lower, upper, total, slots, send_sem, recv_sem, part_sems
):
    blk, tp = lax.axis_index("blk"), lax.axis_index("tp")
    count = blk_count * tp_count
    me = blk * tp_count + tp
    mesh_type = pl.DeviceIdType.MESH
    barrier = pltpu.get_barrier_semaphore()

    def device(distance):
        flat = lax.rem(me + distance, count)
        return (flat // tp_count, lax.rem(flat, tp_count))

    def greet(distance, carry):
        pl.semaphore_signal(barrier, inc=1, device_id=device(distance), device_id_type=mesh_type)
        return carry

    lax.fori_loop(1, count, greet, 0)
    pl.semaphore_wait(barrier, count - 1)
    after = lax.rem(blk + 1, blk_count)
    before = lax.rem(blk + blk_count - 1, blk_count)
    up = pltpu.make_async_remote_copy(
        values, lower, send_sem.at[0], recv_sem.at[0], device_id=(after, tp), device_id_type=mesh_type
    )
    down = pltpu.make_async_remote_copy(
        values, upper, send_sem.at[1], recv_sem.at[1], device_id=(before, tp), device_id_type=mesh_type
    )
    up.start()
    down.start()

    def send(distance, carry):
        pltpu.make_async_remote_copy(
            part,
            slots.at[distance - 1],
            part_sems.at[0],
            part_sems.at[1],
            device_id=device(distance),
            device_id_type=mesh_type,
        ).start()
        return carry

    lax.fori_loop(1, count, send, 0)
    pltpu.make_async_copy(slots, slots, part_sems.at[1]).wait()
    pltpu.make_async_copy(slots, slots, part_sems.at[0]).wait()
    total[...] = jnp.sum(slots[...], axis=0) + part[...]
    up.wait()
    down.wait()


def gossip(values, part):
    blk_count, tp_count = lax.axis_size("blk"), lax.axis_size("tp")
    same = jax.ShapeDtypeStruct(values.shape, values.dtype)
    return pl.pallas_call(
        functools.partial(gossip_kernel, blk_count, tp_count),
        out_shape=(same, same, jax.ShapeDtypeStruct(part.shape, part.dtype)),
        in_specs=[VMEM, VMEM],
        out_specs=(VMEM, VMEM, VMEM),
        scratch_shapes=[
            pltpu.VMEM((blk_count * tp_count - 1,) + part.shape, part.dtype),
            pltpu.SemaphoreType.DMA((2,)),
            pltpu.SemaphoreType.DMA((2,)),
            pltpu.SemaphoreType.DMA((2,)),
        ],
        compiler_params=pltpu.CompilerParams(collective_id=0, has_side_effects=True),
        cost_estimate=pl.CostEstimate(flops=10000, bytes_accessed=10000000, transcendentals=0),
    )(values, part)


def attend(lows, total_rows, qs, ks, vs, og, qg, ids_col, ids_row, bias):
    width = qs.shape[1]
    pair = 2 * HD
    lane = lax.broadcasted_iota(jnp.int32, (1, pair), 1)
    first = jnp.where(lane < HD, 1.0, 0.0).astype(jnp.bfloat16)
    second = jnp.where(lane < HD, 0.0, 1.0).astype(jnp.bfloat16)
    reach = SEG_MOST - 1
    for low in lows:
        start = max(0, (low - reach) // TILE * TILE)
        end = min(total_rows, -(-(low + TILE + reach) // TILE) * TILE)
        span = end - start
        same = ids_col[low : low + TILE, :] == ids_row[:, start:end]
        tile_bias = jnp.where(same, 0.0, -1e30)
        bias[:TILE, :span] = tile_bias
        bias[TILE:, :span] = tile_bias

        @pl.loop(0, width // pair, unroll=2 if width // pair % 2 == 0 else 1)
        def _(index):
            columns = pl.ds(pl.multiple_of(index * pair, pair), pair)
            query = qs[low : low + TILE, columns]
            outer = og[low : low + TILE, columns]
            keyed = ks[start:end, columns]
            valued = vs[start:end, columns]
            queries = jnp.concatenate([query * first, query * second], axis=0)
            outers = jnp.concatenate([outer * first, outer * second], axis=0)
            scores = contract(queries, keyed, 1, 1) + bias[:, :span]
            out_proj = contract(outers, valued, 1, 1)
            exponent = jnp.exp(scores - jnp.max(scores, axis=-1, keepdims=True))
            inverse = 1.0 / jnp.sum(exponent, axis=-1, keepdims=True)
            centre = jnp.sum(exponent * out_proj, axis=-1, keepdims=True) * inverse
            score_grad = (exponent * ((out_proj - centre) * (inverse * HD ** (-0.5)))).astype(
                jnp.bfloat16
            )
            both = jnp.dot(score_grad, keyed, preferred_element_type=jnp.float32)
            qg[low : low + TILE, columns] = jnp.where(lane < HD, both[:TILE], both[TILE:]).astype(
                jnp.bfloat16
            )


def project(start, steps, tok, qw, kw, vw, qs, ks, vs, proj):
    @pl.loop(0, steps)
    def _(step):
        rows = pl.ds(pl.multiple_of(start + step * proj, proj), proj)
        block = tok[rows, :]
        query = jnp.dot(block, qw[...], preferred_element_type=jnp.float32).astype(jnp.bfloat16)
        qs[rows, :] = (query.astype(jnp.float32) * HD ** (-0.5)).astype(jnp.bfloat16)
        ks[rows, :] = jnp.dot(block, kw[...], preferred_element_type=jnp.float32).astype(jnp.bfloat16)
        vs[rows, :] = jnp.dot(block, vw[...], preferred_element_type=jnp.float32).astype(jnp.bfloat16)


def piece_rows(index, rank, local, count):
    start = lax.rem(rank - index + count, count) * local
    return pl.ds(pl.multiple_of(start, local), local)


def span_limit(total_rows):
    return min(total_rows, TILE + 2 * (-(-(SEG_MOST - 1) // TILE) * TILE))


def gradient_kernel(count, *refs):
    pieces = refs[:count]
    (query_w, key_w, value_w, out_grad, ids_col, ids_row, picks_row, picks_col) = refs[count : count + 8]
    fields = refs[count + 8 : count + 12]
    grad_out, tracker_out, copy_out, kept = refs[count + 12 : count + 16]
    scratch = refs[count + 16 :]
    tok, qw, kw, vw, og, tr, tm, tc, gp, qs, ks, vs, qg, upd, bias, go, to, co, tok_sems, sems, out_sems = scratch
    total_rows, model_width = tok.shape
    rank = lax.axis_index("tp")

    loads = []
    for shift in range(count):
        where = piece_rows(shift, rank, pieces[0].shape[0], count)
        loads.append(pltpu.make_async_copy(pieces[shift], tok.at[where], tok_sems.at[shift]))
    sources = (query_w, key_w, value_w, out_grad) + fields
    for index, (source, target) in enumerate(zip(sources, (qw, kw, vw, og, tr, tm, tc, gp))):
        loads.append(pltpu.make_async_copy(source, target, sems.at[index]))
    for load in loads:
        load.start()
    for load in loads[: count + 4]:
        load.wait()

    project(0, total_rows // 256, tok, qw, kw, vw, qs, ks, vs, 256)
    attend(range(0, total_rows, TILE), total_rows, qs, ks, vs, og, qg, ids_col, ids_row, bias)

    for load in loads[count + 4 :]:
        load.wait()

    @pl.loop(0, model_width // TILE)
    def _(step):
        base = pl.multiple_of(step * TILE, TILE)
        rows = pl.ds(base, TILE)
        product = contract(tok[:, rows], qg[...], 0, 0)
        grad = (product * model_width ** (-0.5)).astype(jnp.bfloat16)
        copy = tc[rows, :].astype(jnp.float32)
        new = (
            tr[rows, :].astype(jnp.float32)
            + mixing_rate * (tm[rows, :].astype(jnp.float32) - copy)
            + grad.astype(jnp.float32)
            - gp[rows, :].astype(jnp.float32)
        ).astype(jnp.bfloat16)
        change = new.astype(jnp.float32) - copy
        index = lax.broadcasted_iota(jnp.int32, (TILE, picks_row.shape[1]), 0) + base
        hits = jnp.where(index == picks_row[...], 1.0, 0.0)
        picked = jnp.max(hits, axis=1, keepdims=True)
        go[rows, :] = grad
        to[rows, :] = new
        co[rows, :] = (copy + change * picked).astype(jnp.bfloat16)
        upd[rows, :] = change.astype(jnp.bfloat16)
        for slot, (source, target) in enumerate(((go, grad_out), (to, tracker_out), (co, copy_out))):
            pltpu.make_async_copy(source.at[rows], target.at[rows], out_sems.at[slot]).start()

    columns = lax.broadcasted_iota(jnp.int32, (picks_col.shape[0], model_width), 1)
    matrix = jnp.where(picks_col[...] == columns, 1.0, 0.0).astype(jnp.bfloat16)
    kept[...] = jnp.dot(matrix, upd[...], preferred_element_type=jnp.float32).astype(jnp.bfloat16)
    for slot, (source, target) in enumerate(((go, grad_out), (to, tracker_out), (co, copy_out))):
        pltpu.make_async_copy(source, target, out_sems.at[slot]).wait()


def gradient_stage(pieces, query_weight, key_weight, value_weight, out_grad, image_row, picks, fields):
    count = len(pieces)
    model_width = pieces[0].shape[1]
    total_rows = out_grad.shape[0]
    width = query_weight.shape[1]
    bf16 = jnp.bfloat16
    field = jax.ShapeDtypeStruct((model_width, width), bf16)
    weight = pltpu.VMEM((model_width, width), bf16)
    row_block = pltpu.VMEM((total_rows, width), bf16)
    return pl.pallas_call(
        functools.partial(gradient_kernel, count),
        out_shape=(field, field, field, jax.ShapeDtypeStruct((picks.shape[0], width), bf16)),
        in_specs=[ANY] * (count + 4) + [VMEM] * 4 + [ANY] * 4,
        out_specs=(ANY, ANY, ANY, VMEM),
        scratch_shapes=[pltpu.VMEM((total_rows, model_width), bf16)]
        + [weight] * 3
        + [row_block]
        + [weight] * 4
        + [row_block] * 4
        + [weight, pltpu.VMEM((2 * TILE, span_limit(total_rows)), jnp.float32)]
        + [weight] * 3
        + [
            pltpu.SemaphoreType.DMA((count,)),
            pltpu.SemaphoreType.DMA((8,)),
            pltpu.SemaphoreType.DMA((3,)),
        ],
        compiler_params=pltpu.CompilerParams(vmem_limit_bytes=56 * 2**20),
        cost_estimate=pl.CostEstimate(
            flops=8 * total_rows * model_width * width + 6 * total_rows * 640 * width,
            bytes_accessed=24 * model_width * width,
            transcendentals=total_rows * 640 * width // HD,
        ),
    )(
        *pieces,
        query_weight,
        key_weight,
        value_weight,
        out_grad,
        image_row.reshape(total_rows, 1),
        image_row.reshape(1, total_rows),
        picks.reshape(1, -1),
        picks.reshape(-1, 1),
        *fields,
    )


IMAGES = 6
PACK = 16
WIDE = 256
QUERY_ROWS = 224
KEY_ROWS = 256
MESH = pl.DeviceIdType.MESH


def token_chunks(local):
    edges = [0]
    for count in range(3, IMAGES):
        need = -(-(count * SEG_MOST - local) // 16) * 16
        edges.append(min(local, max(need, edges[-1])))
    edges.insert(-1, edges[-1] - 2 * PACK)
    edges.append(local)
    return list(zip(edges[:-1], edges[1:]))


def pick_column(picks, blk, stream):
    row = picks[blk, stream : stream + 1, :].astype(jnp.float32)
    size = row.shape[1]
    rows = lax.broadcasted_iota(jnp.int32, (size, size), 0)
    columns = lax.broadcasted_iota(jnp.int32, (size, size), 1)
    return jnp.sum(jnp.where(rows == columns, row, 0.0), axis=1, keepdims=True)


def hot_rows(column, total_rows):
    index = lax.broadcasted_iota(jnp.int32, (column.shape[0], total_rows), 1)
    return jnp.where(column == index.astype(jnp.float32), 1.0, 0.0).astype(jnp.bfloat16)


def picked_mask(picks, blk, stream, base, rows):
    row = picks[blk, stream : stream + 1, :]
    index = lax.broadcasted_iota(jnp.int32, (rows, row.shape[1]), 0) + base
    return jnp.max(jnp.where(index == row, 1.0, 0.0), axis=1, keepdims=True)


def window_start(low, ref, rows):
    return jnp.minimum(low // PACK, ref.shape[0] - rows // PACK)


def window(ref, block, rows, columns):
    parts = [ref[block + index, :, columns] for index in range(rows // PACK)]
    return jnp.concatenate(parts, axis=0)


def attend_image(slot, low, high, qs, ks, vs, og, qg, staged):
    width = qs.shape[2]
    pair = 2 * HD
    lane = lax.broadcasted_iota(jnp.int32, (1, pair), 1)
    first = jnp.where(lane < HD, 1.0, 0.0).astype(jnp.bfloat16)
    second = jnp.where(lane < HD, 0.0, 1.0).astype(jnp.bfloat16)
    scale = jnp.bfloat16(HD ** (-0.5))
    first_scaled, second_scaled = first * scale, second * scale
    query_block = window_start(low, qs, QUERY_ROWS)
    key_block = window_start(low, qs, KEY_ROWS)
    position = lax.broadcasted_iota(jnp.int32, (1, KEY_ROWS), 1) + key_block * PACK
    bias = jnp.where((position >= low) & (position < high), 0.0, -1e30)
    row = lax.broadcasted_iota(jnp.int32, (QUERY_ROWS, pair), 0) + query_block * PACK
    inside = (row >= low) & (row < high)

    def start(index):
        columns = pl.ds(index * pair, pair)
        query = window(qs, query_block, QUERY_ROWS, columns)
        outer = window(og, query_block, QUERY_ROWS, columns)
        keyed = window(ks, key_block, KEY_ROWS, columns)
        valued = window(vs, key_block, KEY_ROWS, columns)
        queries = jnp.concatenate([query * first, query * second], axis=0)
        outers = jnp.concatenate([outer * first_scaled, outer * second_scaled], axis=0)
        staged[2 * (index % 2)] = contract(queries, keyed, 1, 1)
        staged[2 * (index % 2) + 1] = contract(outers, valued, 1, 1)

    def finish(index):
        columns = pl.ds(index * pair, pair)
        keyed = window(ks, key_block, KEY_ROWS, columns)
        scores = staged[2 * (index % 2)] + bias
        out_proj = staged[2 * (index % 2) + 1]
        exponent = jnp.exp(scores - jnp.max(scores, axis=-1, keepdims=True))
        inverse = 1.0 / jnp.sum(exponent, axis=-1, keepdims=True)
        centre = jnp.sum(exponent * out_proj, axis=-1, keepdims=True) * inverse
        score_grad = (exponent * ((out_proj - centre) * inverse)).astype(jnp.bfloat16)
        both = jnp.dot(score_grad, keyed, preferred_element_type=jnp.float32)
        merged = jnp.where(lane < HD, both[:QUERY_ROWS], both[QUERY_ROWS:])
        qg[slot, :, columns] = jnp.where(inside, merged, 0.0).astype(jnp.bfloat16)

    pairs = width // pair
    start(0)
    for index in range(pairs):
        if index + 1 < pairs:
            start(index + 1)
        finish(index)


def step_kernel(blk_count, chunks, *refs):
    (weights, copies, mixed, tracker, tracker_copy, tracker_mixed, grad_prev) = refs[:7]
    (tokens, ids, key_weight, value_weight, out_grad, row_picks) = refs[7:13]
    (w_out, copy_out, mix_out, grad_out, new_out, held_out, tm, values, spread, total) = refs[13:23]
    (wt, cp, mx, tr, tc, gp, kw, vw, og, qw, upd, tok, recv) = refs[23:36]
    (qs, ks, vs, qg, acc, base, id_row, picks, heard, hot, part, slots, group, other) = refs[36:50]
    selected, base_rows, copy_rows, grad_rows, staged = refs[50:55]
    (load_sem, send_tok, recv_tok, near, rise, fall, send_row, recv_row, sum_sem) = refs[55:]

    blk, tp = lax.axis_index("blk"), lax.axis_index("tp")
    planes = blk_count // 4
    plane = blk // 4
    blocks = tokens.shape[0]
    width = qs.shape[2]
    model_width = tok.shape[2]
    kept = row_picks.shape[2]
    partner = (blk, 1 - tp)
    after = (lax.rem(blk + 1, blk_count), tp)
    before = (lax.rem(blk + blk_count - 1, blk_count), tp)
    flip_two = (blk + 2 - 4 * (lax.rem(blk, 4) // 2), tp)
    flip_one = (blk + 1 - 2 * lax.rem(blk, 2), tp)
    below = (jnp.maximum(blk - 4, 0), tp)
    above = (jnp.minimum(blk + 4, blk_count - 1), tp)
    lowest = plane == 0
    highest = plane == planes - 1

    barrier = pltpu.get_barrier_semaphore()
    for device in (partner, flip_one, flip_two):
        pl.semaphore_signal(barrier, inc=1, device_id=device, device_id_type=MESH)

    def tell(lower, upper):
        @pl.when(jnp.logical_not(lowest))
        def _():
            pl.semaphore_signal(lower, inc=1, device_id=below, device_id_type=MESH)

        @pl.when(jnp.logical_not(highest))
        def _():
            pl.semaphore_signal(upper, inc=1, device_id=above, device_id_type=MESH)

    def hear(lower, upper):
        @pl.when(jnp.logical_not(highest))
        def _():
            pl.semaphore_wait(lower, 1)

        @pl.when(jnp.logical_not(lowest))
        def _():
            pl.semaphore_wait(upper, 1)

    tell(barrier, barrier)

    own = pl.ds(tp * blocks, blocks)
    far = pl.ds((1 - tp) * blocks, blocks)
    sources = (tokens, row_picks, ids, weights, copies, mixed, tracker)
    sources += (key_weight, value_weight, out_grad, tracker_copy, tracker_mixed, grad_prev)
    targets = (tok.at[own], picks, id_row, wt, cp, mx, tr, kw, vw, og, tc, tm, gp)
    loads = [
        pltpu.make_async_copy(source, target, load_sem.at[index])
        for index, (source, target) in enumerate(zip(sources, targets))
    ]
    for load in loads:
        load.start()
    pl.semaphore_wait(barrier, 5 - lowest.astype(jnp.int32) - highest.astype(jnp.int32))

    sends = []
    for index, (start, end) in enumerate(chunks):
        size = end - start
        first = jnp.where(tp == 0, blocks - end, start)
        send = pltpu.make_async_remote_copy(
            tokens.at[pl.ds(first, size)],
            recv.at[start:end],
            send_tok.at[index],
            recv_tok.at[index],
            device_id=partner,
            device_id_type=MESH,
        )
        send.start()
        sends.append(send)

    pl.semaphore_signal(near.at[0], inc=1, device_id=flip_two, device_id_type=MESH)

    for target in (qs, ks, vs, tok, selected):
        target[far] = jnp.zeros((blocks,) + target.shape[1:], jnp.bfloat16)
    for load in loads[:7]:
        load.wait()

    for stream, target in enumerate((hot, spread)):
        for index, shift in enumerate((blk_count - 1, 0, 1)):
            rank = lax.rem(blk + shift, blk_count)
            target[index * kept : (index + 1) * kept, :] = hot_rows(
                pick_column(picks, rank, stream), model_width
            )

    @pl.loop(0, model_width // TILE)
    def _(step):
        start = pl.multiple_of(step * TILE, TILE)
        rows = pl.ds(start, TILE)
        copy = cp[rows, :].astype(jnp.float32)
        new = (
            wt[rows, :]
            + mixing_rate * (mx[rows, :].astype(jnp.float32) - copy)
            - step_rate * tr[rows, :].astype(jnp.float32)
        )
        change = new - copy
        w_out[rows, :] = new
        query = (new * model_width ** (-0.5)).astype(jnp.bfloat16)
        qw[rows, :] = query * jnp.bfloat16(HD ** (-0.5))
        upd[rows, :] = change.astype(jnp.bfloat16)
        picked = picked_mask(picks, blk, 0, start, TILE)
        copy_out[rows, :] = jnp.where(picked > 0.5, copy + change, copy).astype(jnp.bfloat16)

    middle = slice(kept, 2 * kept)
    heard[middle, :] = jnp.dot(
        hot[middle, :], upd[...], preferred_element_type=jnp.float32
    ).astype(jnp.bfloat16)

    pl.semaphore_wait(near.at[0], 1)
    pl.semaphore_signal(near.at[1], inc=1, device_id=flip_one, device_id_type=MESH)

    edge = []
    for image in range(IMAGES + 1):
        edge.append(jnp.sum(jnp.where(id_row[...] < image, 1, 0)))

    def bounds(slot):
        low = jnp.where(tp == 0, edge[slot], edge[IMAGES - 1 - slot])
        high = jnp.where(tp == 0, edge[slot + 1], edge[IMAGES - slot])
        return low, high

    def project_block(block, rows):
        flat = block.reshape(-1, model_width)
        for target, weight in ((qs, qw), (ks, kw), (vs, vw)):
            result = jnp.dot(flat, weight[...], preferred_element_type=jnp.float32)
            target[rows] = result.astype(jnp.bfloat16).reshape(-1, PACK, width)
        columns = contract(flat, spread[middle, :], 1, 1)
        selected[rows] = columns.astype(jnp.bfloat16).reshape(-1, PACK, kept)

    loads[7].wait()
    loads[8].wait()

    @pl.loop(0, 2)
    def _(step):
        rows = pl.ds(tp * blocks + step * (blocks // 2), blocks // 2)
        project_block(tok[rows], rows)

    pl.semaphore_wait(near.at[1], 1)
    for stage in range(planes - 2):
        tell(fall.at[stage], rise.at[stage])
        if stage == 0:
            loads[9].wait()
            attend_image(0, *bounds(0), qs, ks, vs, og, qg, staged)
        if stage == 1:
            attend_image(1, *bounds(1), qs, ks, vs, og, qg, staged)
        hear(fall.at[stage], rise.at[stage])
    if planes < 3:
        loads[9].wait()
    for slot in range(min(2, planes - 2), 2):
        attend_image(slot, *bounds(slot), qs, ks, vs, og, qg, staged)

    def swap(source, target, index):
        moves = []
        for way, (device, slot) in enumerate(((after, 0), (before, 2))):
            move = pltpu.make_async_remote_copy(
                source.at[middle],
                target.at[slot * kept : (slot + 1) * kept],
                send_row.at[2 * index + way],
                recv_row.at[2 * index + way],
                device_id=device,
                device_id_type=MESH,
            )
            move.start()
            moves.append(move)
        return moves

    param = swap(heard, heard, 0)

    def take(index):
        start, end = chunks[index]
        size = end - start
        sends[index].wait_recv()
        first = blocks * (1 - tp) + jnp.where(tp == 0, start, blocks - end)
        rows = pl.ds(first, size)
        block = recv[start:end]
        tok[rows] = block
        project_block(block, rows)

    take(0)
    attend_image(2, *bounds(2), qs, ks, vs, og, qg, staged)

    for load in loads[10:]:
        load.wait()

    @pl.loop(0, model_width // TILE)
    def _(step):
        rows = pl.ds(pl.multiple_of(step * TILE, TILE), TILE)
        copy = tc[rows, :].astype(jnp.float32)
        base[rows, :] = (
            tr[rows, :].astype(jnp.float32)
            + mixing_rate * (tm[rows, :].astype(jnp.float32) - copy)
            - gp[rows, :].astype(jnp.float32)
        )

    def rows_of(source):
        return jnp.dot(spread[middle, :], source[...], preferred_element_type=jnp.float32)

    copy_rows[...] = rows_of(tc)
    base_rows[...] = (
        rows_of(tr) + mixing_rate * (rows_of(tm) - copy_rows[...]) - rows_of(gp)
    )

    for move in param:
        move.wait()
    part[...] = jnp.zeros_like(part)

    @pl.loop(0, model_width // WIDE)
    def _(step):
        rows = pl.ds(pl.multiple_of(step * WIDE, WIDE), WIDE)
        gain = contract(hot[:, rows], heard[...], 0, 0) / 3.0
        new = (mx[rows, :].astype(jnp.float32) + gain).astype(jnp.bfloat16)
        mix_out[rows, :] = new
        gap = new.astype(jnp.float32) - copy_out[rows, :].astype(jnp.float32)
        square = gap * gap
        folded = sum(square[:, at : at + 128] for at in range(0, width, 128))
        part[...] += jnp.sum(folded.reshape(WIDE // 8, 8, 128), axis=0)

    slots[pl.ds(blk, 1)] = part[...][None]

    def share(distance):
        return pltpu.make_async_remote_copy(
            part,
            slots.at[blk],
            sum_sem.at[0],
            sum_sem.at[1],
            device_id=(lax.rem(blk + distance, blk_count), tp),
            device_id_type=MESH,
        )

    @pl.loop(1, blk_count)
    def _(distance):
        share(distance).start()


    take(1)
    attend_image(3, *bounds(3), qs, ks, vs, og, qg, staged)

    def product(source, slots_used, columns):
        result = 0.0
        for slot in slots_used:
            block = window_start(bounds(slot)[0], source, QUERY_ROWS)
            result += contract(window(source, block, QUERY_ROWS, columns), qg[slot], 0, 0)
        return result

    grad_rows[...] = product(selected, range(4), slice(None))

    @pl.loop(0, model_width // WIDE)
    def _(step):
        rows = pl.ds(pl.multiple_of(step * WIDE, WIDE), WIDE)
        acc[rows, :] = product(tok, range(4), rows)

    take(2)
    take(3)
    attend_image(4, *bounds(4), qs, ks, vs, og, qg, staged)
    take(4)
    attend_image(5, *bounds(5), qs, ks, vs, og, qg, staged)

    gradient = grad_rows[...] + product(selected, (4, 5), slice(None))
    grad = (gradient * model_width ** (-0.5)).astype(jnp.bfloat16)
    new = (base_rows[...] + grad.astype(jnp.float32)).astype(jnp.bfloat16)
    values[middle, :] = (new.astype(jnp.float32) - copy_rows[...]).astype(jnp.bfloat16)
    track = swap(values, values, 1)

    most = pl.ds(0, blk_count - 1)
    for way in range(2):
        pltpu.make_async_copy(slots.at[most], slots.at[most], sum_sem.at[way]).wait()
    group[...] = jnp.sum(slots[...], axis=0)
    cross = pltpu.make_async_remote_copy(
        group, other, sum_sem.at[2], sum_sem.at[3], device_id=partner, device_id_type=MESH
    )
    cross.start()

    @pl.loop(0, model_width // WIDE)
    def _(step):
        start = pl.multiple_of(step * WIDE, WIDE)
        rows = pl.ds(start, WIDE)
        gradient = acc[rows, :] + product(tok, (4, 5), rows)
        grad = (gradient * model_width ** (-0.5)).astype(jnp.bfloat16)
        copy = tc[rows, :].astype(jnp.float32)
        new = (base[rows, :] + grad.astype(jnp.float32)).astype(jnp.bfloat16)
        change = new.astype(jnp.float32) - copy
        picked = picked_mask(picks, blk, 1, start, WIDE)
        grad_out[rows, :] = grad
        new_out[rows, :] = new
        held_out[rows, :] = jnp.where(picked > 0.5, copy + change, copy).astype(jnp.bfloat16)

    cross.wait()
    total[...] = group[...] + other[...]
    for send in sends:
        send.wait_send()
    for move in track:
        move.wait()


def finish_kernel(entries, *refs):
    sources, tm, values, spread, total = refs[:6], refs[6], refs[7], refs[8], refs[9]
    targets, mix_target, sum_target = refs[10:16], refs[16], refs[17]
    mixed, sems = refs[18:]
    model_width = tm.shape[0]
    moves = [
        pltpu.make_async_copy(source, target, sems.at[index])
        for index, (source, target) in enumerate(zip(sources, targets))
    ]
    for move in moves:
        move.start()

    @pl.loop(0, model_width // (2 * TILE))
    def _(step):
        rows = pl.ds(pl.multiple_of(step * 2 * TILE, 2 * TILE), 2 * TILE)
        gain = contract(spread[:, rows], values[...], 0, 0) / 3.0
        mixed[rows, :] = (tm[rows, :].astype(jnp.float32) + gain).astype(jnp.bfloat16)
        pltpu.make_async_copy(mixed.at[rows], mix_target.at[rows], sems.at[6]).start()

    sum_target[...] = jnp.full((1, 1), 0.0, jnp.float32) + jnp.sum(total[...]) / entries
    for move in moves:
        move.wait()
    pltpu.make_async_copy(mixed, mix_target, sems.at[6]).wait()


def fused_step(blk_count, arrays):
    (weights, _, _, _, _, _, _) = arrays[:7]
    (tokens, ids, key_weight, value_weight, out_grad, row_picks) = arrays[7:]
    model_width, width = weights.shape
    packed_tokens = tokens.reshape(-1, PACK, model_width)
    packed_grad = out_grad.reshape(-1, PACK, width)
    arrays = arrays[:7] + (packed_tokens, ids, key_weight, value_weight, packed_grad, row_picks)
    local = tokens.shape[0]
    total_rows = ids.shape[1]
    kept = row_picks.shape[2]
    chunks = [(start // PACK, end // PACK) for start, end in token_chunks(local)]
    planes = blk_count // 4
    bf16, f32 = jnp.bfloat16, jnp.float32
    field = pltpu.VMEM((model_width, width), bf16)
    wide = pltpu.VMEM((model_width, width), f32)
    rows = pltpu.VMEM((total_rows // PACK, PACK, width), bf16)
    lanes = pltpu.VMEM((8, 128), f32)
    heard = pltpu.VMEM((3 * kept, width), bf16)
    hot = pltpu.VMEM((3 * kept, model_width), bf16)
    dma = pltpu.SemaphoreType.DMA
    held = pl.pallas_call(
        functools.partial(step_kernel, blk_count, chunks),
        out_shape=(wide,) + (field,) * 6 + (heard, hot, lanes),
        in_specs=[HBM] * 13,
        out_specs=(VMEM,) * 10,
        scratch_shapes=[wide]
        + [field] * 7
        + [rows, field, field]
        + [pltpu.VMEM((count // PACK, PACK, model_width), bf16) for count in (total_rows, local)]
        + [rows] * 3
        + [pltpu.VMEM((IMAGES, QUERY_ROWS, width), bf16), wide, wide]
        + [pltpu.VMEM(ids.shape, jnp.int32), pltpu.VMEM(row_picks.shape, jnp.int32), heard, hot]
        + [lanes, pltpu.VMEM((blk_count, 8, 128), f32), lanes, lanes]
        + [pltpu.VMEM((total_rows // PACK, PACK, kept), bf16)]
        + [pltpu.VMEM((kept, width), f32)] * 3
        + [pltpu.VMEM((4, 2 * QUERY_ROWS, KEY_ROWS), f32)]
        + [dma((13,)), dma((len(chunks),)), dma((len(chunks),))]
        + [pltpu.SemaphoreType.REGULAR((2,))]
        + [pltpu.SemaphoreType.REGULAR((max(planes - 2, 1),))] * 2
        + [dma((4,)), dma((4,)), dma((4,))],
        compiler_params=pltpu.CompilerParams(
            collective_id=0, has_side_effects=True, vmem_limit_bytes=44 * 2**20
        ),
        cost_estimate=pl.CostEstimate(
            flops=8 * total_rows * model_width * width,
            bytes_accessed=24 * model_width * width,
            transcendentals=total_rows * 256 * width // HD,
        ),
    )(*(pltpu.with_memory_space_constraint(array, pltpu.HBM) for array in arrays))
    flat = jax.ShapeDtypeStruct((model_width, width), bf16)
    entries = float(blk_count * model_width * model_width)
    outs = pl.pallas_call(
        functools.partial(finish_kernel, entries),
        out_shape=(jax.ShapeDtypeStruct((model_width, width), f32),)
        + (flat,) * 6
        + (jax.ShapeDtypeStruct((1, 1), f32),),
        in_specs=[VMEM] * 10,
        out_specs=(HBM,) * 7 + (VMEM,),
        scratch_shapes=[field, dma((7,))],
        compiler_params=pltpu.CompilerParams(vmem_limit_bytes=8 * 2**20),
        cost_estimate=pl.CostEstimate(
            flops=model_width * width * 400,
            bytes_accessed=16 * model_width * width,
            transcendentals=0,
        ),
    )(*held)
    weights_new, copies_new, mixed_new, grad_new, tracker_new, held_new, mixed_back, total = outs
    return (
        weights_new[None],
        copies_new[None],
        mixed_new[None],
        tracker_new[None],
        held_new[None],
        mixed_back[None],
        grad_new[None],
        total[0, 0],
    )


def fits_fused(blk_count, local, model_width, width):
    enough = (IMAGES - 1) * SEG_MOST <= 2 * local and 2 * SEG_MOST <= local <= 3 * SEG_MOST
    shapes = local % 256 == 0 and model_width % 256 == 0 and width % (4 * HD) == 0
    return enough and shapes and blk_count % 4 == 0 and blk_count >= 8


def device_step(
    weights,
    copies,
    copies_mixed,
    tracker,
    tracker_copy,
    tracker_mixed,
    grad_prev,
    tokens,
    image_ids,
    key_weight,
    value_weight,
    out_grad,
    row_picks,
):
    model_width = weights.shape[1]
    blk_count, tp_count = lax.axis_size("blk"), lax.axis_size("tp")
    local = tokens.shape[1]
    if tp_count == 2 and fits_fused(blk_count, local, *weights.shape[1:]):
        fields = (weights, copies, copies_mixed, tracker, tracker_copy, tracker_mixed, grad_prev)
        return fused_step(
            blk_count,
            tuple(field[0] for field in fields)
            + (tokens[0], image_ids, key_weight, value_weight, out_grad[0], row_picks),
        )
    pieces = [tokens[0]]
    for shift in range(1, tp_count):
        hop = [(i, (i + shift) % tp_count) for i in range(tp_count)]
        pieces.append(lax.ppermute(tokens[0], "tp", hop))
    own_picks = replica_picks(row_picks, 0)
    copy_value = copies[0].astype(jnp.float32)
    mixed_value = copies_mixed[0].astype(jnp.float32)
    weights_new = (
        weights[0]
        + mixing_rate * (mixed_value - copy_value)
        - step_rate * tracker[0].astype(jnp.float32)
    )
    query_weight = (weights_new * model_width ** (-0.5)).astype(jnp.bfloat16)
    update = weights_new - copy_value
    picked = picked_rows(own_picks[0], model_width)
    copies_new = jnp.where(picked, copy_value + update, copy_value).astype(jnp.bfloat16)
    kept = contract(
        one_hot(own_picks[0], model_width), update.astype(jnp.bfloat16), 1, 0
    ).astype(jnp.bfloat16)
    up = [(i, (i + 1) % blk_count) for i in range(blk_count)]
    down = [(j, i) for i, j in up]
    lower = lax.ppermute(kept, "blk", up)
    upper = lax.ppermute(kept, "blk", down)
    mixed_new = (
        mixed_value + mix_stream([lower, kept, upper], row_picks, 0, model_width)
    ).astype(jnp.bfloat16)
    gap = mixed_new.astype(jnp.float32) - copies_new.astype(jnp.float32)
    part = jnp.broadcast_to(jnp.sum(gap * gap)[None, None], (8, 128))

    part, query_weight = lax.optimization_barrier((part, query_weight))
    grad_new, tracker_new, tracker_copy_new, kept = gradient_stage(
        pieces,
        query_weight,
        key_weight,
        value_weight,
        out_grad[0],
        image_ids[0],
        own_picks[1],
        (tracker[0], tracker_mixed[0], tracker_copy[0], grad_prev[0]),
    )
    lower, upper, total = gossip(kept, part)
    tracker_mixed_new = (
        tracker_mixed[0].astype(jnp.float32)
        + mix_stream([lower, kept, upper], row_picks, 1, model_width)
    ).astype(jnp.bfloat16)
    entries = float(blk_count * model_width * model_width)
    return (
        weights_new[None],
        copies_new[None],
        mixed_new[None],
        tracker_new[None],
        tracker_copy_new[None],
        tracker_mixed_new[None],
        grad_new[None],
        total[0, 0] / entries,
    )


def solution(mesh):
    field = P("blk", None, "tp")
    return jax.shard_map(
        device_step,
        mesh=mesh,
        in_specs=(field,) * 7
        + (P("blk", "tp", None), P("blk", None), P(None, "tp"), P(None, "tp"), field, P()),
        out_specs=(field,) * 7 + (P(),),
        check_vma=False,
    )
```
